256 devices in a mesh: dp: 8 (over y, x_hi), centers: 32 (over z, x_lo, core).
Axes of the slice: x: 4 (x_hi: 2, x_lo: 2; x = x_hi * 2 + x_lo), y: 4, z: 8, core: 2. Of those that a mesh axis runs over, the one named last changes fastest.
Arguments:
- points: bfloat16 [32768, 32], P('dp'), may hold values from -6 to 6
- centers: bfloat16 [65536, 32], P('centers'), may hold values from -6 to 6
- coef: bfloat16 [65536, 64], P('centers'), may hold values from -0.09375 to 0.09375
Outputs:
- product: float32 [65536, 64], P('centers')
The draws below stay inside these ranges and needn't reach their ends.
All inputs are finite; a program needn't handle non-finite values.
Results may differ from the reference program's by a relative error of at most 0.0003.
Values may be sent and summed in bfloat16 or wider, within the bound.
A program may use at most 128 MiB of HBM per device.

```python
import jax
import jax.numpy as jnp
from jax import lax

DIM = 32
OUTS = 64
NPTS = 32768
CENTERS = 65536


def block_scale(key, shape, shards, low, top_value):
    gain, own = 1.0, jax.random.fold_in(key, 6)
    for axis_at, blocks in shards:
        heights = jnp.exp(jax.random.uniform(jax.random.fold_in(own, axis_at), (blocks,), jnp.float32, low / len(shards), top_value / len(shards)))
        gain = gain * jnp.repeat(heights, shape[axis_at] // blocks).reshape([-1 if axis == axis_at else 1 for axis in range(len(shape))])
    return gain


def scatter_about(rng, shape, scale, limit, cuts=(), kind=jnp.bfloat16):
    values = jax.random.normal(rng, shape, jnp.float32) * scale
    if len(cuts) > 0:
        values = block_scale(rng, shape, cuts, -0.22, 0.18) * values
    return jnp.clip(values, min=-limit, max=limit).astype(kind)


def setup_inputs(seed: int = 0) -> dict:
    key_list = jax.random.split(jax.random.key(seed), 4)
    return {
        "points": scatter_about(key_list[0], (NPTS, DIM), 1.0, 6.0, ((0, 8),)),
        "centers": scatter_about(key_list[1], (CENTERS, DIM), 1.0, 6.0, ((0, 32),)),
        "coef": scatter_about(key_list[2], (CENTERS, OUTS), (CENTERS // 16) ** -0.5, 0.09375, ((0, 32),)),
    }


def kernel_block(left_pts, left_sq, right_pts, right_sq, features):
    inner = lax.dot_general(left_pts, right_pts, (((1,), (1,)), ((), ())), preferred_element_type=jnp.float32)
    dist = left_sq[:, None] + right_sq[None, :] - 2.0 * inner
    return jnp.exp(dist * (-2.0 / features)).astype(jnp.bfloat16)

def squares(values):
    wide = values.astype(jnp.float32)
    return lax.optimization_barrier(jnp.sum(wide * wide, axis=1))

def reference(points, centers, coef):
    features = points.shape[1]
    total_pts = points.shape[0]
    total_cen = centers.shape[0]
    outs_count = coef.shape[1]
    block_pts = min(1024, total_pts)
    cen_sq = squares(centers)
    point_blocks = points.reshape(total_pts // block_pts, block_pts, features)

    def data_step(accum, block):
        kernel = kernel_block(block, squares(block), centers, cen_sq, features)
        forward = jnp.dot(kernel, coef, preferred_element_type=jnp.float32).astype(jnp.bfloat16)
        back = lax.dot_general(kernel, forward, (((0,), (0,)), ((), ())), preferred_element_type=jnp.float32)
        return (accum + back, jnp.zeros((), jnp.float32))
    accum, unused = lax.scan(data_step, jnp.zeros((total_cen, outs_count), jnp.float32), point_blocks)
    block_cen = min(1024, total_cen)
    center_blocks = centers.reshape(total_cen // block_cen, block_cen, features)

    def center_step(carry, block):
        kernel = kernel_block(block, squares(block), centers, cen_sq, features)
        return (carry, jnp.dot(kernel, coef, preferred_element_type=jnp.float32))
    unused_two, regular = lax.scan(center_step, jnp.zeros((), jnp.float32), center_blocks)
    regular = regular.reshape(total_cen, outs_count)
    return accum * (1.0 / jnp.sqrt(jnp.float32(total_pts))) + regular
```

```python
import math

import jax
import jax.numpy as jnp
import numpy as np
from jax import lax
from jax.experimental import pallas as pl
from jax.experimental.pallas import tpu as pltpu
from jax.sharding import PartitionSpec as P

F32, BF16 = jnp.float32, jnp.bfloat16
MESH = pl.DeviceIdType.MESH
ROWS = 128
TILE = 256
CHUNKS = 2


def split3(x):
    a = x.astype(BF16)
    r = x - a.astype(F32)
    b = r.astype(BF16)
    return a, b, (r - b.astype(F32)).astype(BF16)


def tail_rows(pieces, first, ones):
    n = pieces[0].shape[1]
    row = lax.broadcasted_iota(jnp.int32, (32, n), 0)
    out = jnp.where((row >= ones) & (row < ones + 3), 1.0, 0.0)
    for k, piece in enumerate(pieces):
        out = jnp.where(row == first + k, piece.astype(F32), out)
    return out.astype(BF16)


def fill(dst, feats, scale, scaled, cols):
    wide = feats.astype(F32)
    squares = split3(-scale * jnp.sum(wide * wide, axis=0, keepdims=True))
    parts = split3((2.0 * scale) * wide) if scaled else (feats,) * 3
    for k in range(3):
        dst[32 * k : 32 * (k + 1), cols] = parts[k]
    dst[96:128, cols] = tail_rows(squares, 3 if scaled else 0, 0 if scaled else 3)


def dot(a, b):
    return jnp.dot(a, b, preferred_element_type=F32)


def dot_nt(a, b):
    return lax.dot_general(a, b, (((1,), (1,)), ((), ())), preferred_element_type=F32)


def kernel(
    feats, outs, n_pts, n_cen, total_pts,
    p_ref, z_ref, out_ref,
    bpts, bown, arow, kt, fpart, zslots, zaug, mmacc, fwd,
    sbuf, dbuf, rsend, rrecv, dsend, drecv, outt,
    a_send, a_recv, d1_send, d1_recv, rs_send, rs_recv, ag_send, ag_recv,
    d2_send, d2_recv, ds_send, ds_recv, dg_send, dg_recv,
):
    scale = math.log2(math.e) * 2.0 / feats
    norm = float(np.float32(1.0) / np.sqrt(np.float32(total_pts)))
    d, c = lax.axis_index("dp"), lax.axis_index("centers")
    core, x_lo, z = c % 2, (c // 2) % 2, c // 4
    chip = c // 2
    y, x_hi = d // 2, d % 2
    half = outs // 2
    r_own = pl.multiple_of(half * core, half)
    r_other = pl.multiple_of(half * (1 - core), half)
    cpts = n_pts // CHUNKS
    share = cpts // 16
    dshare = n_cen // 8

    def at(dp, cen):
        return {"dp": dp, "centers": cen}

    partner = at(d, chip * 2 + 1 - core)
    x_next = at(d, z * 4 + (1 - x_lo) * 2 + core)

    def chip_peer(k):
        return (chip + k) % 16

    def group(k):
        return at(d, chip_peer(k) * 2 + core)

    def dp_peer(k):
        return (d + k) % 8

    def remote(src, dst, send, recv, dev):
        return pltpu.make_async_remote_copy(
            src_ref=src, dst_ref=dst, send_sem=send, recv_sem=recv, device_id=dev, device_id_type=MESH
        )

    barrier = pltpu.get_barrier_semaphore()
    for k in range(1, 16):
        pl.semaphore_signal(barrier, inc=1, device_id=group(k), device_id_type=MESH)
    pl.semaphore_signal(barrier, inc=1, device_id=partner, device_id_type=MESH)
    for k in range(1, 8):
        pl.semaphore_signal(barrier, inc=1, device_id=at(dp_peer(k), c), device_id_type=MESH)

    def prep_own(t, _):
        cols = pl.ds(pl.multiple_of(t * TILE, TILE), TILE)
        fill(bown, z_ref[0:feats, cols], scale, True, cols)
        arow[cols, :] = bown[:, cols].T
        return 0

    lax.fori_loop(0, n_cen // TILE, prep_own, 0)
    pl.semaphore_wait(barrier, 23)

    dz = (y + 4 * ((x_hi + core) % 2)) % 8
    a0 = remote(z_ref, zslots.at[0], a_send.at[0], a_recv.at[0], at(d, ((z + 8 - dz) % 8) * 4 + x_lo * 2 + core))
    a0_local = pltpu.make_async_copy(z_ref, zslots.at[0], a_recv.at[0])
    a1 = remote(zslots.at[0], zslots.at[1], a_send.at[1], a_recv.at[1], x_next)
    a2 = remote(zslots.at[0], zslots.at[2], a_send.at[2], a_recv.at[2], partner)
    a3 = remote(zslots.at[1], zslots.at[3], a_send.at[3], a_recv.at[3], partner)

    @pl.when(dz != 0)
    def _():
        a0.start()

    @pl.when(dz == 0)
    def _():
        a0_local.start()

    def prep_pts(t, _):
        cols = pl.ds(pl.multiple_of(t * 512, 512), 512)
        fill(bpts, p_ref[:, cols], scale, False, cols)
        return 0

    lax.fori_loop(0, n_pts // 512, prep_pts, 0)

    def nm_step(t, _):
        cols = pl.ds(pl.multiple_of(t * TILE, TILE), TILE)
        right = bpts[:, cols]
        acc = None
        for b in range(n_cen // TILE):
            rows = pl.ds(b * TILE, TILE)
            tile = jnp.exp2(dot(arow[rows, :], right)).astype(BF16)
            kt[rows, cols] = tile
            one = dot(z_ref[feats : feats + outs, rows], tile)
            acc = one if acc is None else acc + one
        fpart[:, cols] = acc
        return 0

    def d1(q):
        return remote(sbuf.at[q], dbuf.at[q], d1_send.at[q], d1_recv.at[q], partner)

    def d1_go(q):
        sbuf[q] = fpart[pl.ds(r_other, half), q * cpts : (q + 1) * cpts].astype(BF16)
        d1(q).start()

    def rs(q, k):
        lanes = pl.ds(pl.multiple_of(chip_peer(k) * share, share), share)
        return remote(rsend.at[q, :, lanes], rrecv.at[q, k], rs_send.at[q, k], rs_recv.at[q, k], group(k))

    def rs_go(q):
        d1(q).wait_recv()
        mine = fpart[pl.ds(r_own, half), q * cpts : (q + 1) * cpts]
        rsend[q] = (mine + dbuf[q].astype(F32)).astype(BF16)
        for k in range(1, 16):
            rs(q, k).start()

    own_rows = pl.ds(r_own, half)

    def ag(q, k):
        where = fwd.at[own_rows, pl.ds(pl.multiple_of(q * cpts + chip * share, share), share)]
        return remote(where, where, ag_send.at[q, k], ag_recv.at[q, k], group(k))

    def ag_go(q):
        total = rsend[q, :, pl.ds(pl.multiple_of(chip * share, share), share)].astype(F32)
        for k in range(1, 16):
            rs(q, k).wait_recv()
            total = total + rrecv[q, k].astype(F32)
        fwd[own_rows, pl.ds(pl.multiple_of(q * cpts + chip * share, share), share)] = total.astype(BF16)
        for k in range(1, 16):
            ag(q, k).start()

    def d2(q):
        where = fwd.at[own_rows, q * cpts : (q + 1) * cpts]
        return remote(where, where, d2_send.at[q], d2_recv.at[q], partner)

    def d2_go(q):
        for k in range(1, 16):
            ag(q, k).wait_recv()
        d2(q).start()

    steps = n_pts // TILE // 4
    lax.fori_loop(0, 2 * steps, nm_step, 0)
    d1_go(0)
    lax.fori_loop(2 * steps, 3 * steps, nm_step, 0)
    rs_go(0)
    lax.fori_loop(3 * steps, 4 * steps, nm_step, 0)
    d1_go(1)

    mmacc[...] = jnp.zeros_like(mmacc)

    def mm_prep(slot):
        def step(t, _):
            cols = pl.ds(pl.multiple_of(t * 512, 512), 512)
            fill(zaug, zslots[slot, 0:feats, cols], scale, False, cols)
            return 0

        lax.fori_loop(0, n_cen // 512, step, 0)

    def mm(slot, lo, hi):
        def step(t, _):
            rows = pl.ds(pl.multiple_of(t * TILE, TILE), TILE)
            left = zaug[:, rows].T
            weights = zslots[slot, feats : feats + outs, rows]
            for b in range(n_cen // TILE):
                cols = pl.ds(b * TILE, TILE)
                tile = jnp.exp2(dot(left, bown[:, cols])).astype(BF16)
                mmacc[:, cols] += dot(weights, tile)
            return 0

        lax.fori_loop(lo, hi, step, 0)

    blocks = n_cen // TILE
    a0_local.wait()
    a1.start()
    a2.start()
    mm_prep(0)
    mm(0, 0, blocks // 2)
    rs_go(1)
    mm(0, blocks // 2, blocks)
    ag_go(0)
    a2.wait_recv()
    mm_prep(2)
    mm(2, 0, blocks)
    ag_go(1)
    a1.wait_recv()
    a3.start()
    mm_prep(1)
    mm(1, 0, blocks)
    d2_go(0)
    a3.wait_recv()
    mm_prep(3)
    mm(3, 0, blocks)
    d2_go(1)
    d2(0).wait_recv()
    d2(1).wait_recv()

    def back(k):
        rows = pl.ds(pl.multiple_of(dp_peer(k) * dshare, dshare), dshare)
        return dot_nt(fwd[...], kt[rows, :]) * norm + mmacc[:, rows]

    def ds_copy(k):
        return remote(dsend.at[k], drecv.at[k], ds_send.at[k], ds_recv.at[k], at(dp_peer(k), c))

    def back_step(k, _):
        dsend[k] = back(k)
        ds_copy(k).start()
        return 0

    lax.fori_loop(1, 8, back_step, 0)
    total = back(0)
    for k in range(1, 8):
        ds_copy(k).wait_recv()
        total = total + drecv[k]
    mine = pl.ds(pl.multiple_of(d * dshare, dshare), dshare)
    outt[:, mine] = total

    def dg(k):
        return remote(outt.at[:, mine], outt.at[:, mine], dg_send.at[k], dg_recv.at[k], at(dp_peer(k), c))

    for k in range(1, 8):
        dg(k).start()

    @pl.when(dz != 0)
    def _():
        a0.wait_send()

    for copy in (a1, a2, a3):
        copy.wait_send()
    for q in range(CHUNKS):
        d1(q).wait_send()
        d2(q).wait_send()
        for k in range(1, 16):
            rs(q, k).wait_send()
            ag(q, k).wait_send()
    for k in range(1, 8):
        ds_copy(k).wait_send()
    for k in range(1, 8):
        dg(k).wait_recv()
    out_ref[...] = outt[...].T
    for k in range(1, 8):
        dg(k).wait_send()


def solution(mesh):
    def on_device(points, centers, coef):
        n_pts, feats = points.shape
        n_cen, outs = coef.shape
        cpts = n_pts // CHUNKS
        dma = pltpu.SemaphoreType.DMA
        stacked = jnp.concatenate((centers, coef), axis=1).T

        def body(*refs):
            kernel(feats, outs, n_pts, n_cen, n_pts * 8, *refs)

        return pl.pallas_call(
            body,
            out_shape=jax.ShapeDtypeStruct((n_cen, outs), F32),
            in_specs=[pl.BlockSpec(memory_space=pltpu.VMEM)] * 2,
            out_specs=pl.BlockSpec(memory_space=pltpu.VMEM),
            scratch_shapes=[
                pltpu.VMEM((ROWS, n_pts), BF16),
                pltpu.VMEM((ROWS, n_cen), BF16),
                pltpu.VMEM((n_cen, ROWS), BF16),
                pltpu.VMEM((n_cen, n_pts), BF16),
                pltpu.VMEM((outs, n_pts), F32),
                pltpu.VMEM((4, feats + outs, n_cen), BF16),
                pltpu.VMEM((ROWS, n_cen), BF16),
                pltpu.VMEM((outs, n_cen), F32),
                pltpu.VMEM((outs, n_pts), BF16),
                pltpu.VMEM((CHUNKS, outs // 2, cpts), BF16),
                pltpu.VMEM((CHUNKS, outs // 2, cpts), BF16),
                pltpu.VMEM((CHUNKS, outs // 2, cpts), BF16),
                pltpu.VMEM((CHUNKS, 16, outs // 2, cpts // 16), BF16),
                pltpu.VMEM((8, outs, n_cen // 8), F32),
                pltpu.VMEM((8, outs, n_cen // 8), F32),
                pltpu.VMEM((outs, n_cen), F32),
                dma((4,)), dma((4,)),
                dma((CHUNKS,)), dma((CHUNKS,)),
                dma((CHUNKS, 16)), dma((CHUNKS, 16)),
                dma((CHUNKS, 16)), dma((CHUNKS, 16)),
                dma((CHUNKS,)), dma((CHUNKS,)),
                dma((8,)), dma((8,)),
                dma((8,)), dma((8,)),
            ],
            compiler_params=pltpu.CompilerParams(
                collective_id=0, has_side_effects=True, vmem_limit_bytes=60 * 1024 * 1024
            ),
        )(points.T, stacked)

    in_specs = (P("dp", None), P("centers", None), P("centers", None))
    return jax.shard_map(
        on_device, mesh=mesh, in_specs=in_specs, out_specs=P("centers", None), check_vma=False
    )
```

```python
import math

import jax
import jax.numpy as jnp
import numpy as np
from jax import lax
from jax.experimental import pallas as pl
from jax.experimental.pallas import tpu as pltpu
from jax.sharding import PartitionSpec as P

F32, BF16 = jnp.float32, jnp.bfloat16
MESH = pl.DeviceIdType.MESH
ROWS = 128
TILE = 256
WIDE = 512
CHUNKS = 2


def split3(x):
    a = x.astype(BF16)
    r = x - a.astype(F32)
    b = r.astype(BF16)
    return a, b, (r - b.astype(F32)).astype(BF16)


def tail_rows(pieces, first, ones):
    n = pieces[0].shape[1]
    row = lax.broadcasted_iota(jnp.int32, (32, n), 0)
    out = jnp.where((row >= ones) & (row < ones + 3), 1.0, 0.0)
    for k, piece in enumerate(pieces):
        out = jnp.where(row == first + k, piece.astype(F32), out)
    return out.astype(BF16)


def fill(dst, feats, scale, scaled, cols):
    wide = feats.astype(F32)
    squares = split3(-scale * jnp.sum(wide * wide, axis=0, keepdims=True))
    parts = split3((2.0 * scale) * wide) if scaled else (feats,) * 3
    for k in range(3):
        dst[32 * k : 32 * (k + 1), cols] = parts[k]
    dst[96:128, cols] = tail_rows(squares, 3 if scaled else 0, 0 if scaled else 3)


def dot(a, b):
    return jnp.dot(a, b, preferred_element_type=F32)


def dot_nt(a, b):
    return lax.dot_general(a, b, (((1,), (1,)), ((), ())), preferred_element_type=F32)


def kernel(
    feats, outs, n_pts, n_cen, total_pts,
    p_ref, z_ref, out_ref,
    bpts, bown, arow, kt, tiles, fpart, zslots, zaug, mmacc, fwd,
    sbuf, dbuf, rsend, rrecv, dsend, drecv, outt,
    a_send, a_recv, d1_send, d1_recv, rs_send, rs_recv, ag_send, ag_recv,
    d2_send, d2_recv, ds_send, ds_recv, dg_send, dg_recv,
):
    scale = math.log2(math.e) * 2.0 / feats
    norm = float(np.float32(1.0) / np.sqrt(np.float32(total_pts)))
    d, c = lax.axis_index("dp"), lax.axis_index("centers")
    core, x_lo, z = c % 2, (c // 2) % 2, c // 4
    chip = c // 2
    y, x_hi = d // 2, d % 2
    half = outs // 2
    r_own = pl.multiple_of(half * core, half)
    r_other = pl.multiple_of(half * (1 - core), half)
    cpts = n_pts // CHUNKS
    share = cpts // 16
    dshare = n_cen // 8

    def at(dp, cen):
        return {"dp": dp, "centers": cen}

    partner = at(d, chip * 2 + 1 - core)
    x_next = at(d, z * 4 + (1 - x_lo) * 2 + core)

    def chip_peer(k):
        return (chip + k) % 16

    def group(k):
        return at(d, chip_peer(k) * 2 + core)

    def dp_peer(k):
        return (d + k) % 8

    def remote(src, dst, send, recv, dev):
        return pltpu.make_async_remote_copy(
            src_ref=src, dst_ref=dst, send_sem=send, recv_sem=recv, device_id=dev, device_id_type=MESH
        )

    barrier = pltpu.get_barrier_semaphore()
    for k in range(1, 16):
        pl.semaphore_signal(barrier, inc=1, device_id=group(k), device_id_type=MESH)
    pl.semaphore_signal(barrier, inc=1, device_id=partner, device_id_type=MESH)
    for k in range(1, 8):
        pl.semaphore_signal(barrier, inc=1, device_id=at(dp_peer(k), c), device_id_type=MESH)

    def prep_own(t, _):
        cols = pl.ds(pl.multiple_of(t * TILE, TILE), TILE)
        fill(bown, z_ref[0:feats, cols], scale, True, cols)
        arow[cols, :] = bown[:, cols].T
        return 0

    with jax.named_scope("prep_own"):
        lax.fori_loop(0, n_cen // TILE, prep_own, 0)
    with jax.named_scope("barrier"):
        pl.semaphore_wait(barrier, 23)

    dz = (y + 4 * ((x_hi + core) % 2)) % 8
    a0 = remote(z_ref, zslots.at[0], a_send.at[0], a_recv.at[0], at(d, ((z + 8 - dz) % 8) * 4 + x_lo * 2 + core))
    a0_local = pltpu.make_async_copy(z_ref, zslots.at[0], a_recv.at[0])
    a1 = remote(zslots.at[0], zslots.at[1], a_send.at[1], a_recv.at[1], partner)
    a2 = remote(zslots.at[0], zslots.at[2], a_send.at[2], a_recv.at[2], x_next)
    a3 = remote(zslots.at[2], zslots.at[3], a_send.at[3], a_recv.at[3], partner)

    @pl.when(dz != 0)
    def _():
        a0.start()

    @pl.when(dz == 0)
    def _():
        a0_local.start()

    def prep_pts(t, _):
        cols = pl.ds(pl.multiple_of(t * 512, 512), 512)
        fill(bpts, p_ref[:, cols], scale, False, cols)
        return 0

    with jax.named_scope("prep_pts"):
        lax.fori_loop(0, n_pts // 512, prep_pts, 0)

    def nm_tiles(t):
        cols = pl.ds(pl.multiple_of(t * WIDE, WIDE), WIDE)
        right = bpts[:, cols]
        for b in range(n_cen // TILE):
            rows = pl.ds(b * TILE, TILE)
            kt[rows, cols] = jnp.exp2(dot(arow[rows, :], right)).astype(BF16)

    def nm_sum(t):
        cols = pl.ds(pl.multiple_of(t * WIDE, WIDE), WIDE)
        fpart[:, cols] = dot(z_ref[feats : feats + outs, :], kt[:, cols])

    def nm_step(t, _):
        nm_sum(t - 1)
        nm_tiles(t)
        return 0

    def d1(q):
        return remote(sbuf.at[q], dbuf.at[q], d1_send.at[q], d1_recv.at[q], partner)

    def d1_go(q):
        sbuf[q] = fpart[pl.ds(r_other, half), q * cpts : (q + 1) * cpts].astype(BF16)
        d1(q).start()

    def rs(q, k):
        lanes = pl.ds(pl.multiple_of(chip_peer(k) * share, share), share)
        return remote(rsend.at[q, :, lanes], rrecv.at[q, k], rs_send.at[q, k], rs_recv.at[q, k], group(k))

    def rs_go(q):
        d1(q).wait_recv()
        mine = fpart[pl.ds(r_own, half), q * cpts : (q + 1) * cpts]
        rsend[q] = (mine + dbuf[q].astype(F32)).astype(BF16)
        for k in range(1, 16):
            rs(q, k).start()

    own_rows = pl.ds(r_own, half)

    def ag(q, k):
        where = fwd.at[own_rows, pl.ds(pl.multiple_of(q * cpts + chip * share, share), share)]
        return remote(where, where, ag_send.at[q, k], ag_recv.at[q, k], group(k))

    def ag_go(q):
        total = rsend[q, :, pl.ds(pl.multiple_of(chip * share, share), share)].astype(F32)
        for k in range(1, 16):
            rs(q, k).wait_recv()
            total = total + rrecv[q, k].astype(F32)
        fwd[own_rows, pl.ds(pl.multiple_of(q * cpts + chip * share, share), share)] = total.astype(BF16)
        for k in range(1, 16):
            ag(q, k).start()

    def d2(q):
        where = fwd.at[own_rows, q * cpts : (q + 1) * cpts]
        return remote(where, where, d2_send.at[q], d2_recv.at[q], partner)

    def d2_go(q):
        for k in range(1, 16):
            ag(q, k).wait_recv()
        d2(q).start()

    steps = n_pts // WIDE
    with jax.named_scope("nm_a"):
        nm_tiles(0)
        lax.fori_loop(1, steps // 2 + 1, nm_step, 0)
    with jax.named_scope("d1_0"):
        d1_go(0)
    with jax.named_scope("nm_b"):
        lax.fori_loop(steps // 2 + 1, steps * 3 // 4, nm_step, 0)
    with jax.named_scope("rs_0"):
        rs_go(0)
    with jax.named_scope("nm_c"):
        lax.fori_loop(steps * 3 // 4, steps, nm_step, 0)
        nm_sum(steps - 1)
    with jax.named_scope("d1_1"):
        d1_go(1)

    mmacc[...] = jnp.zeros_like(mmacc)
    blocks = n_cen // WIDE

    def mm_prep(slot):
        def step(t, _):
            cols = pl.ds(pl.multiple_of(t * 512, 512), 512)
            fill(zaug, zslots[slot, 0:feats, cols], scale, False, cols)
            return 0

        lax.fori_loop(0, n_cen // 512, step, 0)

    def mm_tiles(g):
        left = zaug[:, pl.ds(pl.multiple_of((g % blocks) * WIDE, WIDE), WIDE)].T
        for b in range(n_cen // TILE):
            cols = pl.ds(b * TILE, TILE)
            tiles[g % 2, :, cols] = jnp.exp2(dot(left, bown[:, cols])).astype(BF16)

    def mm_sum(g):
        rows = pl.ds(pl.multiple_of((g % blocks) * WIDE, WIDE), WIDE)
        weights = zslots[g // blocks, feats : feats + outs, rows]
        for b in range(n_cen // TILE):
            cols = pl.ds(b * TILE, TILE)
            mmacc[:, cols] += dot(weights, tiles[g % 2, :, cols])

    def mm_step(g, _):
        mm_sum(g - 1)
        mm_tiles(g)
        return 0

    def mm(lo, hi):
        lax.fori_loop(lo, hi, mm_step, 0)

    with jax.named_scope("a0_wait"):
        a0_local.wait()
    a1.start()
    a2.start()
    with jax.named_scope("mm_a"):
        mm_prep(0)
        mm_tiles(0)
        mm(1, blocks // 2)
    with jax.named_scope("rs_1"):
        rs_go(1)
    with jax.named_scope("mm_b"):
        mm(blocks // 2, blocks)
    with jax.named_scope("ag_0"):
        ag_go(0)
    with jax.named_scope("a1_wait"):
        a1.wait_recv()
    with jax.named_scope("mm_c"):
        mm_prep(1)
        mm(blocks, 2 * blocks)
    with jax.named_scope("ag_1"):
        ag_go(1)
    with jax.named_scope("a2_wait"):
        a2.wait_recv()
    a3.start()
    with jax.named_scope("mm_d"):
        mm_prep(2)
        mm(2 * blocks, 3 * blocks)
    with jax.named_scope("d2_0"):
        d2_go(0)
    with jax.named_scope("a3_wait"):
        a3.wait_recv()
    with jax.named_scope("mm_e"):
        mm_prep(3)
        mm(3 * blocks, 4 * blocks)
        mm_sum(4 * blocks - 1)
    with jax.named_scope("d2_1"):
        d2_go(1)
    with jax.named_scope("d2_wait"):
        d2(0).wait_recv()
        d2(1).wait_recv()

    def back(k):
        rows = pl.ds(pl.multiple_of(dp_peer(k) * dshare, dshare), dshare)
        return dot_nt(fwd[...], kt[rows, :]) * norm + mmacc[:, rows]

    def ds_copy(k):
        return remote(dsend.at[k], drecv.at[k], ds_send.at[k], ds_recv.at[k], at(dp_peer(k), c))

    def back_step(k, _):
        dsend[k] = back(k)
        ds_copy(k).start()
        return 0

    with jax.named_scope("back"):
        lax.fori_loop(1, 8, back_step, 0)
    with jax.named_scope("back0_dswait"):
        total = back(0)
        for k in range(1, 8):
            ds_copy(k).wait_recv()
            total = total + drecv[k]
    mine = pl.ds(pl.multiple_of(d * dshare, dshare), dshare)
    outt[:, mine] = total

    def dg(k):
        return remote(outt.at[:, mine], outt.at[:, mine], dg_send.at[k], dg_recv.at[k], at(dp_peer(k), c))

    for k in range(1, 8):
        dg(k).start()

    @pl.when(dz != 0)
    def _():
        a0.wait_send()

    for copy in (a1, a2, a3):
        copy.wait_send()
    for q in range(CHUNKS):
        d1(q).wait_send()
        d2(q).wait_send()
        for k in range(1, 16):
            rs(q, k).wait_send()
            ag(q, k).wait_send()
    for k in range(1, 8):
        ds_copy(k).wait_send()
    with jax.named_scope("dg_wait_out"):
        for k in range(1, 8):
            dg(k).wait_recv()
        out_ref[...] = outt[...].T
    for k in range(1, 8):
        dg(k).wait_send()


def solution(mesh):
    def on_device(points, centers, coef):
        n_pts, feats = points.shape
        n_cen, outs = coef.shape
        cpts = n_pts // CHUNKS
        dma = pltpu.SemaphoreType.DMA
        stacked = jnp.concatenate((centers, coef), axis=1).T

        def body(*refs):
            kernel(feats, outs, n_pts, n_cen, n_pts * 8, *refs)

        return pl.pallas_call(
            body,
            out_shape=jax.ShapeDtypeStruct((n_cen, outs), F32),
            in_specs=[pl.BlockSpec(memory_space=pltpu.VMEM)] * 2,
            out_specs=pl.BlockSpec(memory_space=pltpu.VMEM),
            scratch_shapes=[
                pltpu.VMEM((ROWS, n_pts), BF16),
                pltpu.VMEM((ROWS, n_cen), BF16),
                pltpu.VMEM((n_cen, ROWS), BF16),
                pltpu.VMEM((n_cen, n_pts), BF16),
                pltpu.VMEM((2, WIDE, n_cen), BF16),
                pltpu.VMEM((outs, n_pts), F32),
                pltpu.VMEM((4, feats + outs, n_cen), BF16),
                pltpu.VMEM((ROWS, n_cen), BF16),
                pltpu.VMEM((outs, n_cen), F32),
                pltpu.VMEM((outs, n_pts), BF16),
                pltpu.VMEM((CHUNKS, outs // 2, cpts), BF16),
                pltpu.VMEM((CHUNKS, outs // 2, cpts), BF16),
                pltpu.VMEM((CHUNKS, outs // 2, cpts), BF16),
                pltpu.VMEM((CHUNKS, 16, outs // 2, cpts // 16), BF16),
                pltpu.VMEM((8, outs, n_cen // 8), F32),
                pltpu.VMEM((8, outs, n_cen // 8), F32),
                pltpu.VMEM((outs, n_cen), F32),
                dma((4,)), dma((4,)),
                dma((CHUNKS,)), dma((CHUNKS,)),
                dma((CHUNKS, 16)), dma((CHUNKS, 16)),
                dma((CHUNKS, 16)), dma((CHUNKS, 16)),
                dma((CHUNKS,)), dma((CHUNKS,)),
                dma((8,)), dma((8,)),
                dma((8,)), dma((8,)),
            ],
            compiler_params=pltpu.CompilerParams(
                collective_id=0, has_side_effects=True, vmem_limit_bytes=60 * 1024 * 1024
            ),
        )(points.T, stacked)

    in_specs = (P("dp", None), P("centers", None), P("centers", None))
    return jax.shard_map(
        on_device, mesh=mesh, in_specs=in_specs, out_specs=P("centers", None), check_vma=False
    )
```

```python
import math

import jax
import jax.numpy as jnp
import numpy as np
from jax import lax
from jax.experimental import pallas as pl
from jax.experimental.pallas import tpu as pltpu
from jax.sharding import PartitionSpec as P

F32, BF16 = jnp.float32, jnp.bfloat16
MESH = pl.DeviceIdType.MESH
ROWS = 128
TILE = 256
WIDE = 512
CHUNKS = 2


def split3(x):
    a = x.astype(BF16)
    r = x - a.astype(F32)
    b = r.astype(BF16)
    return a, b, (r - b.astype(F32)).astype(BF16)


def tail_rows(pieces, first, ones):
    n = pieces[0].shape[1]
    row = lax.broadcasted_iota(jnp.int32, (32, n), 0)
    out = jnp.where((row >= ones) & (row < ones + 3), 1.0, 0.0)
    for k, piece in enumerate(pieces):
        out = jnp.where(row == first + k, piece.astype(F32), out)
    return out.astype(BF16)


def fill(dst, feats, scale, scaled, cols):
    wide = feats.astype(F32)
    squares = split3(-scale * jnp.sum(wide * wide, axis=0, keepdims=True))
    parts = split3((2.0 * scale) * wide) if scaled else (feats,) * 3
    for k in range(3):
        dst[32 * k : 32 * (k + 1), cols] = parts[k]
    dst[96:128, cols] = tail_rows(squares, 3 if scaled else 0, 0 if scaled else 3)


def dot(a, b):
    return jnp.dot(a, b, preferred_element_type=F32)


def dot_nt(a, b):
    return lax.dot_general(a, b, (((1,), (1,)), ((), ())), preferred_element_type=F32)


def kernel(
    feats, outs, n_pts, n_cen, total_pts,
    p_ref, z_ref, out_ref,
    bpts, bown, arow, kta, ktb, tilea, tileb, fpart, zslots, zaug, mmacc, fwd,
    sbuf, dbuf, rsend, rrecv, dsend, drecv, outt,
    a_send, a_recv, d1_send, d1_recv, rs_send, rs_recv, ag_send, ag_recv,
    d2_send, d2_recv, ds_send, ds_recv, dg_send, dg_recv,
):
    scale = math.log2(math.e) * 2.0 / feats
    norm = float(np.float32(1.0) / np.sqrt(np.float32(total_pts)))
    d, c = lax.axis_index("dp"), lax.axis_index("centers")
    core, x_lo, z = c % 2, (c // 2) % 2, c // 4
    chip = c // 2
    y, x_hi = d // 2, d % 2
    kts, tiles = (kta, ktb), (tilea, tileb)
    half = outs // 2
    r_own = pl.multiple_of(half * core, half)
    r_other = pl.multiple_of(half * (1 - core), half)
    cpts = n_pts // CHUNKS
    share = cpts // 16
    dshare = n_cen // 8

    def at(dp, cen):
        return {"dp": dp, "centers": cen}

    partner = at(d, chip * 2 + 1 - core)
    x_next = at(d, z * 4 + (1 - x_lo) * 2 + core)

    def chip_peer(k):
        return (chip + k) % 16

    def group(k):
        return at(d, chip_peer(k) * 2 + core)

    def dp_peer(k):
        return (d + k) % 8

    def remote(src, dst, send, recv, dev):
        return pltpu.make_async_remote_copy(
            src_ref=src, dst_ref=dst, send_sem=send, recv_sem=recv, device_id=dev, device_id_type=MESH
        )

    barrier = pltpu.get_barrier_semaphore()
    for k in range(1, 16):
        pl.semaphore_signal(barrier, inc=1, device_id=group(k), device_id_type=MESH)
    pl.semaphore_signal(barrier, inc=1, device_id=partner, device_id_type=MESH)
    for k in range(1, 8):
        pl.semaphore_signal(barrier, inc=1, device_id=at(dp_peer(k), c), device_id_type=MESH)

    def prep_own(t, _):
        cols = pl.ds(pl.multiple_of(t * TILE, TILE), TILE)
        fill(bown, z_ref[0:feats, cols], scale, True, cols)
        arow[cols, :] = bown[:, cols].T
        return 0

    def prep_pts(t, _):
        cols = pl.ds(pl.multiple_of(t * 512, 512), 512)
        for e in range(2):
            fill(bpts.at[e], p_ref[:, pl.ds(pl.multiple_of(e * (n_pts // 2) + t * 512, 512), 512)], scale, False, cols)
        return 0

    with jax.named_scope("prep"):
        lax.fori_loop(0, n_cen // TILE, prep_own, 0)
        lax.fori_loop(0, n_pts // 1024, prep_pts, 0)

    dz = (y + 4 * ((x_hi + core) % 2)) % 8
    far = jnp.where((dz >= 3) & (dz <= 6), 1, 0)
    hcen = n_cen // 2

    def part(ref, h):
        return ref.at[:, h * hcen : (h + 1) * hcen]

    def a_z(h):
        dest = at(d, ((z + 8 - dz) % 8) * 4 + x_lo * 2 + core)
        return remote(part(z_ref, h), part(zslots.at[2 * far], h), a_send.at[0, h], a_recv.at[2 * far, h], dest)

    def a_local(h):
        return pltpu.make_async_copy(part(z_ref, h), part(zslots.at[2 * far], h), a_recv.at[2 * far, h])

    def a_x(slot, h):
        return remote(part(zslots.at[slot], h), part(zslots.at[slot + 1], h), a_send.at[1, h], a_recv.at[slot + 1, h], x_next)

    def a_core(slot, h):
        where = part(zslots.at[slot], h)
        return remote(where, where, a_send.at[2 + slot % 2, h], a_recv.at[slot, h], partner)

    def a_arrived(slot, h):
        where = part(zslots.at[slot], h)
        pltpu.make_async_copy(where, where, a_recv.at[slot, h]).wait()

        @pl.when(far == slot // 2)
        def _():
            a_core(slot, h).start()
            if slot % 2 == 0:
                a_x(slot, h).start()

    def nm_tiles(t, ref):
        cols = pl.ds(pl.multiple_of(t * WIDE, WIDE), WIDE)
        right = bpts[ref, :, cols]
        for b in range(n_cen // TILE):
            rows = pl.ds(b * TILE, TILE)
            kts[ref][rows, cols] = jnp.exp2(dot(arow[rows, :], right)).astype(BF16)

    def nm_sum(t, ref):
        cols = pl.ds(pl.multiple_of(t * WIDE, WIDE), WIDE)
        fpart[ref, :, cols] = dot(z_ref[feats : feats + outs, :], kts[ref][:, cols])

    def nm_step(t, first):
        if not first:
            nm_sum(t - 1, 1)
        nm_tiles(t, 0)
        nm_sum(t, 0)
        nm_tiles(t, 1)

    def nm(lo, hi):
        def step(t, _):
            nm_step(t, False)
            return 0

        lax.fori_loop(lo, hi, step, 0)

    piece = cpts // 2

    def d1(q):
        return remote(sbuf.at[q], dbuf.at[q], d1_send.at[q], d1_recv.at[q], partner)

    def d1_go(q):
        for e in range(2):
            sbuf[q, :, e * piece : (e + 1) * piece] = fpart[e, pl.ds(r_other, half), q * piece : (q + 1) * piece].astype(BF16)
        d1(q).start()

    def rs(q, k):
        lanes = pl.ds(pl.multiple_of(chip_peer(k) * share, share), share)
        return remote(rsend.at[q, :, lanes], rrecv.at[q, k], rs_send.at[q, k], rs_recv.at[q, k], group(k))

    own_rows = pl.ds(r_own, half)

    def rs_go(q):
        d1(q).wait_recv()
        for e in range(2):
            lanes = slice(e * piece, (e + 1) * piece)
            mine = fpart[e, own_rows, q * piece : (q + 1) * piece]
            rsend[q, :, lanes] = (mine + dbuf[q, :, lanes].astype(F32)).astype(BF16)
        for k in range(1, 16):
            rs(q, k).start()

    def own_share(q):
        return (chip // 8, own_rows, pl.ds(pl.multiple_of(q * piece + (chip % 8) * share, share), share))

    def ag(q, k):
        where = fwd.at[own_share(q)]
        return remote(where, where, ag_send.at[q, k], ag_recv.at[q, k], group(k))

    def ag_go(q):
        total = rsend[q, :, pl.ds(pl.multiple_of(chip * share, share), share)].astype(F32)
        for k in range(1, 16):
            rs(q, k).wait_recv()
            total = total + rrecv[q, k].astype(F32)
        fwd[own_share(q)] = total.astype(BF16)
        for k in range(1, 16):
            ag(q, k).start()

    def d2(q):
        where = fwd.at[:, own_rows, q * piece : (q + 1) * piece]
        return remote(where, where, d2_send.at[q], d2_recv.at[q], partner)

    def d2_go(q):
        for k in range(1, 16):
            ag(q, k).wait_recv()
        d2(q).start()

    blocks = n_cen // WIDE // 2

    def mm_prep(slot, h):
        def step(t, _):
            cols = pl.ds(pl.multiple_of(t * 512, 512), 512)
            fill(zaug, zslots[slot, 0:feats, cols], scale, False, cols)
            return 0

        lax.fori_loop(h * hcen // 512, (h + 1) * hcen // 512, step, 0)

    def mm_tiles(g, ref):
        start = (g % blocks) * (2 * WIDE) + ref * WIDE
        left = zaug[:, pl.ds(pl.multiple_of(start, WIDE), WIDE)].T
        for b in range(n_cen // TILE):
            cols = pl.ds(b * TILE, TILE)
            tiles[ref][:, cols] = jnp.exp2(dot(left, bown[:, cols])).astype(BF16)

    def mm_sum(slot, g, ref, first=False):
        start = (g % blocks) * (2 * WIDE) + ref * WIDE
        weights = zslots[slot, feats : feats + outs, pl.ds(pl.multiple_of(start, WIDE), WIDE)]
        for b in range(n_cen // TILE):
            cols = pl.ds(b * TILE, TILE)
            one = dot(weights, tiles[ref][:, cols])
            mmacc[:, cols] = one if first else mmacc[:, cols] + one

    def mm(body, last):
        slot, h = body
        mm_prep(slot, h)
        if last is not None:
            mm_sum(*last, 1)
        mm_tiles(h, 0)
        mm_sum(slot, h, 0, first=last is None)
        mm_tiles(h, 1)

    with jax.named_scope("nm_a"):
        nm_step(0, True)
    with jax.named_scope("barrier"):
        pl.semaphore_wait(barrier, 23)

    @pl.when(dz != 0)
    def _():
        for h in range(2):
            a_z(h).start()

    @pl.when(dz == 0)
    def _():
        for h in range(2):
            a_local(h).start()

    steps = n_pts // WIDE // 2
    with jax.named_scope("nm_b"):
        nm(1, steps // 2 + 1)
    with jax.named_scope("d1_0"):
        d1_go(0)
    with jax.named_scope("nm_c"):
        nm(steps // 2 + 1, steps)
        nm_sum(steps - 1, 1)
    with jax.named_scope("d1_1"):
        d1_go(1)
    with jax.named_scope("rs_0"):
        rs_go(0)
    order = [(0, 0), (0, 1), (1, 0), (1, 1), (2, 0), (3, 0), (2, 1), (3, 1)]
    after = {0: lambda: rs_go(1), 1: lambda: ag_go(0), 3: lambda: ag_go(1), 5: lambda: d2_go(0), 6: lambda: d2_go(1)}
    early = {2: [(2, 0)], 5: [(2, 1)]}
    done = set()
    for n, body in enumerate(order):
        with jax.named_scope(f"a_{n}"):
            for what in early.get(n, []) + [body]:
                if what not in done:
                    a_arrived(*what)
                    done.add(what)
        with jax.named_scope(f"mm_{n}"):
            mm(body, order[n - 1] if n else None)
        if n in after:
            with jax.named_scope(f"after_{n}"):
                after[n]()
    with jax.named_scope("mm_end"):
        mm_sum(*order[-1], 1)
    with jax.named_scope("d2_wait"):
        d2(0).wait_recv()
        d2(1).wait_recv()

    def back(k):
        rows = pl.ds(pl.multiple_of(dp_peer(k) * dshare, dshare), dshare)
        total = dot_nt(fwd[0], kta[rows, :]) + dot_nt(fwd[1], ktb[rows, :])
        return total * norm + mmacc[:, rows]

    def ds_copy(k):
        return remote(dsend.at[k], drecv.at[k], ds_send.at[k], ds_recv.at[k], at(dp_peer(k), c))

    def back_step(k, _):
        dsend[k] = back(k)
        ds_copy(k).start()
        return 0

    with jax.named_scope("back"):
        lax.fori_loop(1, 8, back_step, 0)
    with jax.named_scope("back0_dswait"):
        total = back(0)
        for k in range(1, 8):
            ds_copy(k).wait_recv()
            total = total + drecv[k]
    mine = pl.ds(pl.multiple_of(d * dshare, dshare), dshare)
    outt[:, mine] = total

    def dg(k):
        return remote(outt.at[:, mine], outt.at[:, mine], dg_send.at[k], dg_recv.at[k], at(dp_peer(k), c))

    for k in range(1, 8):
        dg(k).start()

    for h in range(2):

        @pl.when(dz != 0)
        def _():
            a_z(h).wait_send()

        a_x(0, h).wait_send()
        a_core(0, h).wait_send()
        a_core(1, h).wait_send()
    for q in range(CHUNKS):
        d1(q).wait_send()
        d2(q).wait_send()
        for k in range(1, 16):
            rs(q, k).wait_send()
            ag(q, k).wait_send()
    for k in range(1, 8):
        ds_copy(k).wait_send()
    with jax.named_scope("dg_wait_out"):
        for k in range(1, 8):
            dg(k).wait_recv()
        out_ref[...] = outt[...].T
    for k in range(1, 8):
        dg(k).wait_send()


def solution(mesh):
    def on_device(points, centers, coef):
        n_pts, feats = points.shape
        n_cen, outs = coef.shape
        cpts = n_pts // CHUNKS
        dma = pltpu.SemaphoreType.DMA
        stacked = jnp.concatenate((centers, coef), axis=1).T

        def body(*refs):
            kernel(feats, outs, n_pts, n_cen, n_pts * 8, *refs)

        return pl.pallas_call(
            body,
            out_shape=jax.ShapeDtypeStruct((n_cen, outs), F32),
            in_specs=[pl.BlockSpec(memory_space=pltpu.VMEM)] * 2,
            out_specs=pl.BlockSpec(memory_space=pltpu.VMEM),
            scratch_shapes=[
                pltpu.VMEM((2, ROWS, n_pts // 2), BF16),
                pltpu.VMEM((ROWS, n_cen), BF16),
                pltpu.VMEM((n_cen, ROWS), BF16),
                pltpu.VMEM((n_cen, n_pts // 2), BF16),
                pltpu.VMEM((n_cen, n_pts // 2), BF16),
                pltpu.VMEM((WIDE, n_cen), BF16),
                pltpu.VMEM((WIDE, n_cen), BF16),
                pltpu.VMEM((2, outs, n_pts // 2), F32),
                pltpu.VMEM((4, feats + outs, n_cen), BF16),
                pltpu.VMEM((ROWS, n_cen), BF16),
                pltpu.VMEM((outs, n_cen), F32),
                pltpu.VMEM((2, outs, n_pts // 2), BF16),
                pltpu.VMEM((CHUNKS, outs // 2, cpts), BF16),
                pltpu.VMEM((CHUNKS, outs // 2, cpts), BF16),
                pltpu.VMEM((CHUNKS, outs // 2, cpts), BF16),
                pltpu.VMEM((CHUNKS, 16, outs // 2, cpts // 16), BF16),
                pltpu.VMEM((8, outs, n_cen // 8), F32),
                pltpu.VMEM((8, outs, n_cen // 8), F32),
                pltpu.VMEM((outs, n_cen), F32),
                dma((4, 2)), dma((4, 2)),
                dma((CHUNKS,)), dma((CHUNKS,)),
                dma((CHUNKS, 16)), dma((CHUNKS, 16)),
                dma((CHUNKS, 16)), dma((CHUNKS, 16)),
                dma((CHUNKS,)), dma((CHUNKS,)),
                dma((8,)), dma((8,)),
                dma((8,)), dma((8,)),
            ],
            compiler_params=pltpu.CompilerParams(
                collective_id=0, has_side_effects=True, vmem_limit_bytes=60 * 1024 * 1024
            ),
        )(points.T, stacked)

    in_specs = (P("dp", None), P("centers", None), P("centers", None))
    return jax.shard_map(
        on_device, mesh=mesh, in_specs=in_specs, out_specs=P("centers", None), check_vma=False
    )
```

```python
import math

import jax
import jax.numpy as jnp
import numpy as np
from jax import lax
from jax.experimental import pallas as pl
from jax.experimental.pallas import tpu as pltpu
from jax.sharding import PartitionSpec as P

F32, BF16 = jnp.float32, jnp.bfloat16
MESH = pl.DeviceIdType.MESH
ROWS = 128
TILE = 256
WIDE = 512
CHUNKS = 2


def split3(x):
    a = x.astype(BF16)
    r = x - a.astype(F32)
    b = r.astype(BF16)
    return a, b, (r - b.astype(F32)).astype(BF16)


def tail_rows(pieces, first, ones):
    n = pieces[0].shape[1]
    row = lax.broadcasted_iota(jnp.int32, (32, n), 0)
    out = jnp.where((row >= ones) & (row < ones + 3), 1.0, 0.0)
    for k, piece in enumerate(pieces):
        out = jnp.where(row == first + k, piece.astype(F32), out)
    return out.astype(BF16)


def fill(dst, feats, scale, scaled, cols):
    wide = feats.astype(F32)
    squares = split3(-scale * jnp.sum(wide * wide, axis=0, keepdims=True))
    parts = split3((2.0 * scale) * wide) if scaled else (feats,) * 3
    for k in range(3):
        dst[32 * k : 32 * (k + 1), cols] = parts[k]
    dst[96:128, cols] = tail_rows(squares, 3 if scaled else 0, 0 if scaled else 3)


def dot(a, b):
    return jnp.dot(a, b, preferred_element_type=F32)


def dot_nt(a, b):
    return lax.dot_general(a, b, (((1,), (1,)), ((), ())), preferred_element_type=F32)


def kernel(
    feats, outs, n_pts, n_cen, total_pts,
    p_ref, z_ref, out_ref,
    bpts, bown, arow, kta, ktb, tilea, tileb, fpart, zbuf, zaug, mmacc, fwd,
    sbuf, dbuf, rsend, rrecv, dsend, drecv, outt,
    z_send, z_recv, x_send, x_recv, c1_send, c1_recv, c3_send, c3_recv,
    d1_send, d1_recv, rs_send, rs_recv, ag_send, ag_recv,
    d2_send, d2_recv, ds_send, ds_recv, dg_send, dg_recv,
):
    scale = math.log2(math.e) * 2.0 / feats
    norm = float(np.float32(1.0) / np.sqrt(np.float32(total_pts)))
    d, c = lax.axis_index("dp"), lax.axis_index("centers")
    core, x_lo, z = c % 2, (c // 2) % 2, c // 4
    chip = c // 2
    y, x_hi = d // 2, d % 2
    kts, tiles = (kta, ktb), (tilea, tileb)
    half = outs // 2
    r_own = pl.multiple_of(half * core, half)
    r_other = pl.multiple_of(half * (1 - core), half)
    cpts = n_pts // CHUNKS
    share = cpts // 16
    dshare = n_cen // 8

    def at(dp, cen):
        return {"dp": dp, "centers": cen}

    partner = at(d, chip * 2 + 1 - core)
    x_next = at(d, z * 4 + (1 - x_lo) * 2 + core)

    def chip_peer(k):
        return (chip + k) % 16

    def group(k):
        return at(d, chip_peer(k) * 2 + core)

    def dp_peer(k):
        return (d + k) % 8

    def remote(src, dst, send, recv, dev):
        return pltpu.make_async_remote_copy(
            src_ref=src, dst_ref=dst, send_sem=send, recv_sem=recv, device_id=dev, device_id_type=MESH
        )

    barrier = pltpu.get_barrier_semaphore()
    for k in range(1, 16):
        pl.semaphore_signal(barrier, inc=1, device_id=group(k), device_id_type=MESH)
    pl.semaphore_signal(barrier, inc=1, device_id=partner, device_id_type=MESH)
    for k in range(1, 8):
        pl.semaphore_signal(barrier, inc=1, device_id=at(dp_peer(k), c), device_id_type=MESH)

    def prep_own(t, _):
        cols = pl.ds(pl.multiple_of(t * TILE, TILE), TILE)
        fill(bown, z_ref[0:feats, cols], scale, True, cols)
        arow[cols, :] = bown[:, cols].T
        return 0

    def prep_pts(t, _):
        cols = pl.ds(pl.multiple_of(t * 512, 512), 512)
        for e in range(2):
            fill(bpts.at[e], p_ref[:, pl.ds(pl.multiple_of(e * (n_pts // 2) + t * 512, 512), 512)], scale, False, cols)
        return 0

    with jax.named_scope("prep"):
        lax.fori_loop(0, n_cen // TILE, prep_own, 0)
        lax.fori_loop(0, n_pts // 1024, prep_pts, 0)

    part = n_cen // 8
    own_part = (slice(None), pl.ds(pl.multiple_of(d * part, part), part))

    def place(slab, pos):
        return zbuf.at[slab, :, pos * part : (pos + 1) * part]

    def a_z(slab):
        up = slab % 2
        dest = at(d, ((z + (1 if up else 7)) % 8) * 4 + x_lo * 2 + core)
        src = z_ref.at[own_part] if slab <= 2 else place(slab - 2, 0)
        return remote(src, place(slab, 0), z_send.at[slab], z_recv.at[slab], dest)

    def a_mine(slab):
        return z_ref.at[own_part] if slab == 0 else place(slab, 0)

    def a_x(slab):
        return remote(a_mine(slab), place(slab, 2), x_send.at[slab], x_recv.at[slab], x_next)

    def a_core(slab):
        return remote(a_mine(slab), place(slab, 1), c1_send.at[slab], c1_recv.at[slab], partner)

    def a_cross(slab):
        return remote(place(slab, 2), place(slab, 3), c3_send.at[slab], c3_recv.at[slab], partner)

    def z_came(slab):
        a_z(slab).wait_recv()
        if slab + 2 <= 7:
            a_z(slab + 2).start()
        a_x(slab).start()
        a_core(slab).start()

    def x_came(slab):
        a_x(slab).wait_recv()
        a_cross(slab).start()

    def slab_ready(slab):
        where = zbuf.at[slab, :, 0:part]
        pltpu.make_async_copy(where, where, c1_recv.at[slab]).wait()
        pltpu.make_async_copy(where, where, c3_recv.at[slab]).wait()

    def nm_tiles(t, ref):
        cols = pl.ds(pl.multiple_of(t * WIDE, WIDE), WIDE)
        right = bpts[ref, :, cols]
        for b in range(n_cen // TILE):
            rows = pl.ds(b * TILE, TILE)
            kts[ref][rows, cols] = jnp.exp2(dot(arow[rows, :], right)).astype(BF16)

    def nm_sum(t, ref):
        cols = pl.ds(pl.multiple_of(t * WIDE, WIDE), WIDE)
        fpart[ref, :, cols] = dot(z_ref[feats : feats + outs, :], kts[ref][:, cols])

    def nm_step(t, first):
        if not first:
            nm_sum(t - 1, 1)
        nm_tiles(t, 0)
        nm_sum(t, 0)
        nm_tiles(t, 1)

    piece = cpts // 2

    def d1(q):
        return remote(sbuf.at[q], dbuf.at[q], d1_send.at[q], d1_recv.at[q], partner)

    def d1_go(q):
        for e in range(2):
            sbuf[q, :, e * piece : (e + 1) * piece] = fpart[e, pl.ds(r_other, half), q * piece : (q + 1) * piece].astype(BF16)
        d1(q).start()

    def rs(q, k):
        lanes = pl.ds(pl.multiple_of(chip_peer(k) * share, share), share)
        return remote(rsend.at[q, :, lanes], rrecv.at[q, k], rs_send.at[q, k], rs_recv.at[q, k], group(k))

    own_rows = pl.ds(r_own, half)

    def rs_go(q):
        d1(q).wait_recv()
        for e in range(2):
            lanes = slice(e * piece, (e + 1) * piece)
            mine = fpart[e, own_rows, q * piece : (q + 1) * piece]
            rsend[q, :, lanes] = (mine + dbuf[q, :, lanes].astype(F32)).astype(BF16)
        for k in range(1, 16):
            rs(q, k).start()

    def own_share(q):
        return (chip // 8, own_rows, pl.ds(pl.multiple_of(q * piece + (chip % 8) * share, share), share))

    def ag(q, k):
        where = fwd.at[own_share(q)]
        return remote(where, where, ag_send.at[q, k], ag_recv.at[q, k], group(k))

    def ag_go(q):
        total = rsend[q, :, pl.ds(pl.multiple_of(chip * share, share), share)].astype(F32)
        for k in range(1, 16):
            rs(q, k).wait_recv()
            total = total + rrecv[q, k].astype(F32)
        fwd[own_share(q)] = total.astype(BF16)
        for k in range(1, 16):
            ag(q, k).start()

    def d2(q):
        where = fwd.at[:, own_rows, q * piece : (q + 1) * piece]
        return remote(where, where, d2_send.at[q], d2_recv.at[q], partner)

    def d2_go(q):
        for k in range(1, 16):
            ag(q, k).wait_recv()
        d2(q).start()

    def mm_prep(slab):
        for h in range(2):
            cols = slice(h * WIDE, (h + 1) * WIDE)
            fill(zaug, zbuf[slab, 0:feats, cols], scale, False, cols)

    def mm_tiles(ref):
        left = zaug[:, ref * WIDE : (ref + 1) * WIDE].T
        for b in range(n_cen // TILE):
            cols = pl.ds(b * TILE, TILE)
            tiles[ref][:, cols] = jnp.exp2(dot(left, bown[:, cols])).astype(BF16)

    def mm_sum(slab, ref, first=False):
        weights = zbuf[slab, feats : feats + outs, ref * WIDE : (ref + 1) * WIDE]
        for b in range(n_cen // TILE):
            cols = pl.ds(b * TILE, TILE)
            one = dot(weights, tiles[ref][:, cols])
            mmacc[:, cols] = one if first else mmacc[:, cols] + one

    def mm(slab, first):
        slab_ready(slab)
        mm_prep(slab)
        if not first:
            mm_sum(slab - 1, 1)
        mm_tiles(0)
        mm_sum(slab, 0, first)
        mm_tiles(1)

    def actions(n, table):
        for step, todo in table.items():

            @pl.when(n == step)
            def _():
                for f, q in todo:
                    f(q)

    steps = n_pts // WIDE // 2
    with jax.named_scope("nm_a"):
        nm_step(0, True)
    with jax.named_scope("barrier"):
        pl.semaphore_wait(barrier, 23)
    a_z(1).start()
    a_z(2).start()
    a_x(0).start()
    a_core(0).start()
    zbuf[0, :, 0:part] = z_ref[own_part]

    def nm_body(n, _):
        with jax.named_scope("nm_body"):
            nm_step(n, False)
        with jax.named_scope("nm_act"):
            actions(n, {2: [(d1_go, 0), (z_came, 1), (z_came, 2), (x_came, 0)]})
        return 0

    lax.fori_loop(1, steps, nm_body, 0)
    with jax.named_scope("nm_end"):
        nm_sum(steps - 1, 1)
    with jax.named_scope("nm_end_act"):
        d1_go(1)
        rs_go(0)
        z_came(3)
        z_came(4)

    with jax.named_scope("mm_0"):
        mm(0, True)
    with jax.named_scope("mm_0_act"):
        rs_go(1)
        z_came(5)
        z_came(6)
        x_came(1)
        x_came(2)

    table = {
        1: [(z_came, 7), (x_came, 3)],
        2: [(ag_go, 0), (x_came, 4)],
        3: [(x_came, 5)],
        4: [(ag_go, 1), (x_came, 6)],
        5: [(x_came, 7), (d2_go, 0)],
        6: [(d2_go, 1)],
    }

    def mm_body(n, _):
        with jax.named_scope("mm_body"):
            mm(n, False)
        with jax.named_scope("mm_act"):
            actions(n, table)
        return 0

    lax.fori_loop(1, 8, mm_body, 0)
    with jax.named_scope("mm_end"):
        mm_sum(7, 1)
    with jax.named_scope("d2_wait"):
        d2(0).wait_recv()
        d2(1).wait_recv()

    def back(k):
        rows = pl.ds(pl.multiple_of(dp_peer(k) * dshare, dshare), dshare)
        total = dot_nt(fwd[0], kta[rows, :]) + dot_nt(fwd[1], ktb[rows, :])
        return total * norm + mmacc[:, rows]

    def ds_copy(k):
        return remote(dsend.at[k], drecv.at[k], ds_send.at[k], ds_recv.at[k], at(dp_peer(k), c))

    def back_step(k, _):
        dsend[k] = back(k)
        ds_copy(k).start()
        return 0

    with jax.named_scope("back"):
        lax.fori_loop(1, 8, back_step, 0)
    with jax.named_scope("back0_dswait"):
        total = back(0)
        for k in range(1, 8):
            ds_copy(k).wait_recv()
            total = total + drecv[k]
    mine = pl.ds(pl.multiple_of(d * dshare, dshare), dshare)
    outt[:, mine] = total

    def dg(k):
        return remote(outt.at[:, mine], outt.at[:, mine], dg_send.at[k], dg_recv.at[k], at(dp_peer(k), c))

    for k in range(1, 8):
        dg(k).start()

    for slab in range(8):
        if slab:
            a_z(slab).wait_send()
        a_x(slab).wait_send()
        a_core(slab).wait_send()
        a_cross(slab).wait_send()
    for q in range(CHUNKS):
        d1(q).wait_send()
        d2(q).wait_send()
        for k in range(1, 16):
            rs(q, k).wait_send()
            ag(q, k).wait_send()
    for k in range(1, 8):
        ds_copy(k).wait_send()
    with jax.named_scope("dg_wait_out"):
        for k in range(1, 8):
            dg(k).wait_recv()
        out_ref[...] = outt[...].T
    for k in range(1, 8):
        dg(k).wait_send()


def solution(mesh):
    def on_device(points, centers, coef):
        n_pts, feats = points.shape
        n_cen, outs = coef.shape
        cpts = n_pts // CHUNKS
        dma = pltpu.SemaphoreType.DMA
        stacked = jnp.concatenate((centers, coef), axis=1).T

        def body(*refs):
            kernel(feats, outs, n_pts, n_cen, n_pts * 8, *refs)

        return pl.pallas_call(
            body,
            out_shape=jax.ShapeDtypeStruct((n_cen, outs), F32),
            in_specs=[pl.BlockSpec(memory_space=pltpu.VMEM)] * 2,
            out_specs=pl.BlockSpec(memory_space=pltpu.VMEM),
            scratch_shapes=[
                pltpu.VMEM((2, ROWS, n_pts // 2), BF16),
                pltpu.VMEM((ROWS, n_cen), BF16),
                pltpu.VMEM((n_cen, ROWS), BF16),
                pltpu.VMEM((n_cen, n_pts // 2), BF16),
                pltpu.VMEM((n_cen, n_pts // 2), BF16),
                pltpu.VMEM((WIDE, n_cen), BF16),
                pltpu.VMEM((WIDE, n_cen), BF16),
                pltpu.VMEM((2, outs, n_pts // 2), F32),
                pltpu.VMEM((8, feats + outs, n_cen // 2), BF16),
                pltpu.VMEM((ROWS, n_cen // 2), BF16),
                pltpu.VMEM((outs, n_cen), F32),
                pltpu.VMEM((2, outs, n_pts // 2), BF16),
                pltpu.VMEM((CHUNKS, outs // 2, cpts), BF16),
                pltpu.VMEM((CHUNKS, outs // 2, cpts), BF16),
                pltpu.VMEM((CHUNKS, outs // 2, cpts), BF16),
                pltpu.VMEM((CHUNKS, 16, outs // 2, cpts // 16), BF16),
                pltpu.VMEM((8, outs, n_cen // 8), F32),
                pltpu.VMEM((8, outs, n_cen // 8), F32),
                pltpu.VMEM((outs, n_cen), F32),
                *[dma((8,))] * 8,
                dma((CHUNKS,)), dma((CHUNKS,)),
                dma((CHUNKS, 16)), dma((CHUNKS, 16)),
                dma((CHUNKS, 16)), dma((CHUNKS, 16)),
                dma((CHUNKS,)), dma((CHUNKS,)),
                dma((8,)), dma((8,)),
                dma((8,)), dma((8,)),
            ],
            compiler_params=pltpu.CompilerParams(
                collective_id=0, has_side_effects=True, vmem_limit_bytes=60 * 1024 * 1024
            ),
        )(points.T, stacked)

    in_specs = (P("dp", None), P("centers", None), P("centers", None))
    return jax.shard_map(
        on_device, mesh=mesh, in_specs=in_specs, out_specs=P("centers", None), check_vma=False
    )
```

```python
import math

import jax
import jax.numpy as jnp
import numpy as np
from jax import lax
from jax.experimental import pallas as pl
from jax.experimental.pallas import tpu as pltpu
from jax.sharding import PartitionSpec as P

F32, BF16 = jnp.float32, jnp.bfloat16
MESH = pl.DeviceIdType.MESH
ROWS = 128
TILE = 256
WIDE = 512
CHUNKS = 2


def split3(x):
    a = x.astype(BF16)
    r = x - a.astype(F32)
    b = r.astype(BF16)
    return a, b, (r - b.astype(F32)).astype(BF16)


def tail_rows(pieces, first, ones):
    n = pieces[0].shape[1]
    row = lax.broadcasted_iota(jnp.int32, (32, n), 0)
    out = jnp.where((row >= ones) & (row < ones + 3), 1.0, 0.0)
    for k, piece in enumerate(pieces):
        out = jnp.where(row == first + k, piece.astype(F32), out)
    return out.astype(BF16)


def fill(dst, feats, scale, scaled, cols):
    wide = feats.astype(F32)
    squares = split3(-scale * jnp.sum(wide * wide, axis=0, keepdims=True))
    parts = split3((2.0 * scale) * wide) if scaled else (feats,) * 3
    for k in range(3):
        dst[32 * k : 32 * (k + 1), cols] = parts[k]
    dst[96:128, cols] = tail_rows(squares, 3 if scaled else 0, 0 if scaled else 3)


def dot(a, b):
    return jnp.dot(a, b, preferred_element_type=F32)


def dot_nt(a, b):
    return lax.dot_general(a, b, (((1,), (1,)), ((), ())), preferred_element_type=F32)


def kernel(
    feats, outs, n_pts, n_cen, total_pts,
    p_ref, c_ref, w_ref, out_ref,
    bpts, bown, arow, kta, ktb, tilea, tileb, fpart, zbuf, zaug, mmacc, fwd,
    sbuf, dbuf, rsend, rrecv, dsend, drecv, outt,
    z_send, z_recv, x_send, x_recv, c1_send, c1_recv, c3_send, c3_recv, own_sem,
    d1_send, d1_recv, rs_send, rs_recv, ag_send, ag_recv,
    d2_send, d2_recv, ds_send, ds_recv, dg_send, dg_recv,
):
    scale = math.log2(math.e) * 2.0 / feats
    norm = float(np.float32(1.0) / np.sqrt(np.float32(total_pts)))
    d, c = lax.axis_index("dp"), lax.axis_index("centers")
    core, x_lo, z = c % 2, (c // 2) % 2, c // 4
    chip = c // 2
    y, x_hi = d // 2, d % 2
    kts, tiles = (kta, ktb), (tilea, tileb)
    half = outs // 2
    r_own = pl.multiple_of(half * core, half)
    r_other = pl.multiple_of(half * (1 - core), half)
    cpts = n_pts // CHUNKS
    share = cpts // 16
    dshare = n_cen // 8

    def at(dp, cen):
        return {"dp": dp, "centers": cen}

    partner = at(d, chip * 2 + 1 - core)
    x_next = at(d, z * 4 + (1 - x_lo) * 2 + core)

    def chip_peer(k):
        return (chip + k) % 16

    def group(k):
        return at(d, chip_peer(k) * 2 + core)

    def dp_peer(k):
        return (d + k) % 8

    def remote(src, dst, send, recv, dev):
        return pltpu.make_async_remote_copy(
            src_ref=src, dst_ref=dst, send_sem=send, recv_sem=recv, device_id=dev, device_id_type=MESH
        )

    barrier = pltpu.get_barrier_semaphore()
    for k in range(1, 16):
        pl.semaphore_signal(barrier, inc=1, device_id=group(k), device_id_type=MESH)
    pl.semaphore_signal(barrier, inc=1, device_id=partner, device_id_type=MESH)
    for k in range(1, 8):
        pl.semaphore_signal(barrier, inc=1, device_id=at(dp_peer(k), c), device_id_type=MESH)

    def prep_own(t, _):
        cols = pl.ds(pl.multiple_of(t * TILE, TILE), TILE)
        fill(bown, c_ref[:, cols], scale, True, cols)
        arow[cols, :] = bown[:, cols].T
        return 0

    def prep_pts(t, _):
        cols = pl.ds(pl.multiple_of(t * 512, 512), 512)
        for e in range(2):
            fill(bpts.at[e], p_ref[:, pl.ds(pl.multiple_of(e * (n_pts // 2) + t * 512, 512), 512)], scale, False, cols)
        return 0

    with jax.named_scope("prep"):
        lax.fori_loop(0, n_cen // TILE, prep_own, 0)
        lax.fori_loop(0, n_pts // 1024, prep_pts, 0)

    part = n_cen // 8
    own_part = pl.ds(pl.multiple_of(d * part, part), part)

    def place(slab, pos):
        if slab in (0, 7):
            body, at_pos = slab, pos
        else:
            first = (slab + 1) // 2 * 2 - 1
            body, at_pos = first + pos // 2, 2 * (slab - first) + pos % 2
        return zbuf.at[body, :, at_pos * part : (at_pos + 1) * part]

    def a_z(slab):
        dest = at(d, ((z + (1 if slab % 2 else 7)) % 8) * 4 + x_lo * 2 + core)
        return remote(place(max(slab - 2, 0), 0), place(slab, 0), z_send.at[slab], z_recv.at[slab], dest)

    def a_x(slab):
        return remote(place(slab, 0), place(slab, 2), x_send.at[slab], x_recv.at[slab], x_next)

    def a_core(slab):
        return remote(place(slab, 0), place(slab, 1), c1_send.at[slab], c1_recv.at[slab], partner)

    def a_cross(slab):
        return remote(place(slab, 2), place(slab, 3), c3_send.at[slab], c3_recv.at[slab], partner)

    def z_came(slab):
        a_z(slab).wait_recv()
        if slab + 2 <= 7:
            a_z(slab + 2).start()
        a_core(slab).start()
        a_x(slab).start()

    def x_came(slab):
        a_x(slab).wait_recv()
        a_cross(slab).start()

    def arrived(body, h):
        if body in (0, 7):
            (a_cross if h else a_core)(body).wait_recv()
        else:
            slab = (body - 1) // 2 * 2 + 1 + h
            (a_core if body % 2 else a_cross)(slab).wait_recv()

    a_own = [
        pltpu.make_async_copy(src.at[:, own_part], zbuf.at[0, lo : lo + src.shape[0], 0:part], own_sem.at[n])
        for n, (src, lo) in enumerate(((c_ref, 0), (w_ref, feats)))
    ]
    for copy in a_own:
        copy.start()

    def nm_tiles(t, ref):
        cols = pl.ds(pl.multiple_of(t * WIDE, WIDE), WIDE)
        right = bpts[ref, :, cols]
        for b in range(n_cen // TILE):
            rows = pl.ds(b * TILE, TILE)
            kts[ref][rows, cols] = jnp.exp2(dot(arow[rows, :], right)).astype(BF16)

    def nm_sum(t, ref):
        cols = pl.ds(pl.multiple_of(t * WIDE, WIDE), WIDE)
        fpart[ref, :, cols] = dot(w_ref[...], kts[ref][:, cols])

    def nm_step(t, first):
        if not first:
            nm_sum(t - 1, 1)
        nm_tiles(t, 0)
        nm_sum(t, 0)
        nm_tiles(t, 1)

    piece = cpts // 2

    def d1(q):
        return remote(sbuf.at[q], dbuf.at[q], d1_send.at[q], d1_recv.at[q], partner)

    def d1_go(q):
        for e in range(2):
            sbuf[q, :, e * piece : (e + 1) * piece] = fpart[e, pl.ds(r_other, half), q * piece : (q + 1) * piece].astype(BF16)
        d1(q).start()

    def rs(q, k):
        lanes = pl.ds(pl.multiple_of(chip_peer(k) * share, share), share)
        return remote(rsend.at[q, :, lanes], rrecv.at[q, k], rs_send.at[q, k], rs_recv.at[q, k], group(k))

    own_rows = pl.ds(r_own, half)

    def rs_go(q):
        d1(q).wait_recv()
        for e in range(2):
            lanes = slice(e * piece, (e + 1) * piece)
            mine = fpart[e, own_rows, q * piece : (q + 1) * piece]
            rsend[q, :, lanes] = (mine + dbuf[q, :, lanes].astype(F32)).astype(BF16)
        for k in range(1, 16):
            rs(q, k).start()

    def own_share(q):
        return (chip // 8, own_rows, pl.ds(pl.multiple_of(q * piece + (chip % 8) * share, share), share))

    def ag(q, k):
        where = fwd.at[own_share(q)]
        return remote(where, where, ag_send.at[q, k], ag_recv.at[q, k], group(k))

    def ag_go(q):
        total = rsend[q, :, pl.ds(pl.multiple_of(chip * share, share), share)].astype(F32)
        for k in range(1, 16):
            rs(q, k).wait_recv()
            total = total + rrecv[q, k].astype(F32)
        fwd[own_share(q)] = total.astype(BF16)
        for k in range(1, 16):
            ag(q, k).start()

    def d2(q):
        where = fwd.at[:, own_rows, q * piece : (q + 1) * piece]
        return remote(where, where, d2_send.at[q], d2_recv.at[q], partner)

    def d2_go(q):
        for k in range(1, 16):
            ag(q, k).wait_recv()
        d2(q).start()

    def mm_tiles(body, ref):
        cols = slice(ref * WIDE, (ref + 1) * WIDE)
        fill(zaug, zbuf[body, 0:feats, cols], scale, False, cols)
        left = zaug[:, cols].T
        for b in range(n_cen // TILE):
            cols = pl.ds(b * TILE, TILE)
            tiles[ref][:, cols] = jnp.exp2(dot(left, bown[:, cols])).astype(BF16)

    def mm_sum(body, ref, first=False):
        weights = zbuf[body, feats : feats + outs, ref * WIDE : (ref + 1) * WIDE]
        for b in range(n_cen // TILE):
            cols = pl.ds(b * TILE, TILE)
            one = dot(weights, tiles[ref][:, cols])
            mmacc[:, cols] = one if first else mmacc[:, cols] + one

    def mm(body, first):
        if not first:
            mm_sum(body - 1, 1)
        mm_tiles(body, 0)
        mm_sum(body, 0, first)
        mm_tiles(body, 1)

    def actions(n, table):
        for step, todo in table.items():

            @pl.when(n == step)
            def _():
                for f, q in todo:
                    f(q)

    steps = n_pts // WIDE // 2
    with jax.named_scope("nm_a"):
        nm_step(0, True)
    with jax.named_scope("barrier"):
        pl.semaphore_wait(barrier, 23)
    for copy in a_own:
        copy.wait()
    a_z(1).start()
    a_z(2).start()
    a_x(0).start()
    a_core(0).start()

    def nm_body(n, _):
        with jax.named_scope("nm_body"):
            nm_step(n, False)
        with jax.named_scope("nm_act"):
            actions(n, {2: [(d1_go, 0), (z_came, 1), (z_came, 2), (x_came, 0)]})
        return 0

    lax.fori_loop(1, steps, nm_body, 0)
    with jax.named_scope("nm_end"):
        nm_sum(steps - 1, 1)
    with jax.named_scope("nm_end_act"):
        d1_go(1)
        rs_go(0)
        arrived(0, 0)
        arrived(0, 1)

    with jax.named_scope("mm_0"):
        mm(0, True)
    with jax.named_scope("mm_0_act"):
        rs_go(1)
        z_came(3)
        z_came(4)
        x_came(1)
        x_came(2)
        arrived(1, 0)
        arrived(1, 1)

    table = {
        1: [],
        2: [(z_came, 5), (z_came, 6), (x_came, 3), (x_came, 4), (ag_go, 0)],
        3: [],
        4: [(z_came, 7), (x_came, 5), (x_came, 6), (ag_go, 1)],
        5: [(d2_go, 0)],
        6: [(x_came, 7), (d2_go, 1)],
    }

    def mm_body(n, _):
        with jax.named_scope("mm_body"):
            mm(n, False)
        with jax.named_scope("mm_act"):
            for step, todo in table.items():

                @pl.when(n == step)
                def _():
                    for f, q in todo:
                        f(q)
                    arrived(step + 1, 0)
                    arrived(step + 1, 1)

        return 0

    lax.fori_loop(1, 8, mm_body, 0)
    with jax.named_scope("mm_end"):
        mm_sum(7, 1)
    with jax.named_scope("d2_wait"):
        d2(0).wait_recv()
        d2(1).wait_recv()

    def back(k):
        rows = pl.ds(pl.multiple_of(dp_peer(k) * dshare, dshare), dshare)
        total = dot_nt(fwd[0], kta[rows, :]) + dot_nt(fwd[1], ktb[rows, :])
        return total * norm + mmacc[:, rows]

    def ds_copy(k):
        return remote(dsend.at[k], drecv.at[k], ds_send.at[k], ds_recv.at[k], at(dp_peer(k), c))

    def back_step(k, _):
        dsend[k] = back(k)
        ds_copy(k).start()
        return 0

    with jax.named_scope("back"):
        lax.fori_loop(1, 8, back_step, 0)
    with jax.named_scope("back0_dswait"):
        total = back(0)
        for k in range(1, 8):
            ds_copy(k).wait_recv()
            total = total + drecv[k]
    mine = pl.ds(pl.multiple_of(d * dshare, dshare), dshare)
    outt[:, mine] = total

    def dg(k):
        return remote(outt.at[:, mine], outt.at[:, mine], dg_send.at[k], dg_recv.at[k], at(dp_peer(k), c))

    for k in range(1, 8):
        dg(k).start()

    for slab in range(8):
        if slab:
            a_z(slab).wait_send()
        a_x(slab).wait_send()
        a_core(slab).wait_send()
        a_cross(slab).wait_send()
    for q in range(CHUNKS):
        d1(q).wait_send()
        d2(q).wait_send()
        for k in range(1, 16):
            rs(q, k).wait_send()
            ag(q, k).wait_send()
    for k in range(1, 8):
        ds_copy(k).wait_send()
    with jax.named_scope("dg_wait_out"):
        for k in range(1, 8):
            dg(k).wait_recv()
        out_ref[...] = outt[...]
    for k in range(1, 8):
        dg(k).wait_send()


def solution(mesh):
    def on_device(points, centers, coef):
        n_pts, feats = points.shape
        n_cen, outs = coef.shape
        cpts = n_pts // CHUNKS
        dma = pltpu.SemaphoreType.DMA

        def body(*refs):
            kernel(feats, outs, n_pts, n_cen, n_pts * 8, *refs)

        return pl.pallas_call(
            body,
            out_shape=jax.ShapeDtypeStruct((outs, n_cen), F32),
            in_specs=[pl.BlockSpec(memory_space=pltpu.VMEM)] * 3,
            out_specs=pl.BlockSpec(memory_space=pltpu.VMEM),
            scratch_shapes=[
                pltpu.VMEM((2, ROWS, n_pts // 2), BF16),
                pltpu.VMEM((ROWS, n_cen), BF16),
                pltpu.VMEM((n_cen, ROWS), BF16),
                pltpu.VMEM((n_cen, n_pts // 2), BF16),
                pltpu.VMEM((n_cen, n_pts // 2), BF16),
                pltpu.VMEM((WIDE, n_cen), BF16),
                pltpu.VMEM((WIDE, n_cen), BF16),
                pltpu.VMEM((2, outs, n_pts // 2), F32),
                pltpu.VMEM((8, feats + outs, n_cen // 2), BF16),
                pltpu.VMEM((ROWS, n_cen // 2), BF16),
                pltpu.VMEM((outs, n_cen), F32),
                pltpu.VMEM((2, outs, n_pts // 2), BF16),
                pltpu.VMEM((CHUNKS, outs // 2, cpts), BF16),
                pltpu.VMEM((CHUNKS, outs // 2, cpts), BF16),
                pltpu.VMEM((CHUNKS, outs // 2, cpts), BF16),
                pltpu.VMEM((CHUNKS, 16, outs // 2, cpts // 16), BF16),
                pltpu.VMEM((8, outs, n_cen // 8), F32),
                pltpu.VMEM((8, outs, n_cen // 8), F32),
                pltpu.VMEM((outs, n_cen), F32),
                *[dma((8,))] * 8, dma((2,)),
                dma((CHUNKS,)), dma((CHUNKS,)),
                dma((CHUNKS, 16)), dma((CHUNKS, 16)),
                dma((CHUNKS, 16)), dma((CHUNKS, 16)),
                dma((CHUNKS,)), dma((CHUNKS,)),
                dma((8,)), dma((8,)),
                dma((8,)), dma((8,)),
            ],
            compiler_params=pltpu.CompilerParams(
                collective_id=0, has_side_effects=True, vmem_limit_bytes=60 * 1024 * 1024
            ),
        )(points.T, centers.T, coef.T).T

    in_specs = (P("dp", None), P("centers", None), P("centers", None))
    return jax.shard_map(
        on_device, mesh=mesh, in_specs=in_specs, out_specs=P("centers", None), check_vma=False
    )
```

```python
import math

import jax
import jax.numpy as jnp
import numpy as np
from jax import lax
from jax.experimental import pallas as pl
from jax.experimental.pallas import tpu as pltpu
from jax.sharding import PartitionSpec as P

F32, BF16 = jnp.float32, jnp.bfloat16
MESH = pl.DeviceIdType.MESH
ROWS = 128
TILE = 256
WIDE = 512
CHUNKS = 2


def split3(x):
    a = x.astype(BF16)
    r = x - a.astype(F32)
    b = r.astype(BF16)
    return a, b, (r - b.astype(F32)).astype(BF16)


def tail_rows(pieces, first, ones):
    n = pieces[0].shape[1]
    row = lax.broadcasted_iota(jnp.int32, (32, n), 0)
    out = jnp.where((row >= ones) & (row < ones + 3), 1.0, 0.0)
    for k, piece in enumerate(pieces):
        out = jnp.where(row == first + k, piece.astype(F32), out)
    return out.astype(BF16)


def fill(dst, feats, scale, scaled, cols):
    wide = feats.astype(F32)
    squares = split3(-scale * jnp.sum(wide * wide, axis=0, keepdims=True))
    parts = split3((2.0 * scale) * wide) if scaled else (feats,) * 3
    for k in range(3):
        dst[32 * k : 32 * (k + 1), cols] = parts[k]
    dst[96:128, cols] = tail_rows(squares, 3 if scaled else 0, 0 if scaled else 3)


def dot(a, b):
    return jnp.dot(a, b, preferred_element_type=F32)


def dot_nt(a, b):
    return lax.dot_general(a, b, (((1,), (1,)), ((), ())), preferred_element_type=F32)


def kernel(
    feats, outs, n_pts, n_cen, total_pts,
    p_ref, c_ref, w_ref, out_ref,
    bpts, bown, arow, kta, ktb, tilea, tileb, fpart, zbuf, zaug, mmacc, fwd,
    sbuf, dbuf, rsend, rrecv, dsend, drecv, outt,
    z_send, z_recv, x_send, x_recv, c1_send, c1_recv, c3_send, c3_recv, own_sem,
    d1_send, d1_recv, rs_send, rs_recv, ag_send, ag_recv,
    d2_send, d2_recv, ds_send, ds_recv, dg_send, dg_recv,
):
    scale = math.log2(math.e) * 2.0 / feats
    norm = float(np.float32(1.0) / np.sqrt(np.float32(total_pts)))
    d, c = lax.axis_index("dp"), lax.axis_index("centers")
    core, x_lo, z = c % 2, (c // 2) % 2, c // 4
    chip = c // 2
    y, x_hi = d // 2, d % 2
    kts, tiles = (kta, ktb), (tilea, tileb)
    half = outs // 2
    r_own = pl.multiple_of(half * core, half)
    r_other = pl.multiple_of(half * (1 - core), half)
    cpts = n_pts // CHUNKS
    share = cpts // 16
    dshare = n_cen // 8

    def at(dp, cen):
        return {"dp": dp, "centers": cen}

    partner = at(d, chip * 2 + 1 - core)
    x_next = at(d, z * 4 + (1 - x_lo) * 2 + core)

    def chip_peer(k):
        return (chip + k) % 16

    def group(k):
        return at(d, chip_peer(k) * 2 + core)

    def dp_peer(k):
        return (d + k) % 8

    def remote(src, dst, send, recv, dev):
        return pltpu.make_async_remote_copy(
            src_ref=src, dst_ref=dst, send_sem=send, recv_sem=recv, device_id=dev, device_id_type=MESH
        )

    barrier = pltpu.get_barrier_semaphore()
    for k in range(1, 16):
        pl.semaphore_signal(barrier, inc=1, device_id=group(k), device_id_type=MESH)
    pl.semaphore_signal(barrier, inc=1, device_id=partner, device_id_type=MESH)
    for k in range(1, 8):
        pl.semaphore_signal(barrier, inc=1, device_id=at(dp_peer(k), c), device_id_type=MESH)

    def prep_own(t, _):
        cols = pl.ds(pl.multiple_of(t * TILE, TILE), TILE)
        fill(bown, c_ref[:, cols], scale, True, cols)
        arow[cols, :] = bown[:, cols].T
        return 0

    def prep_pts(t, _):
        cols = pl.ds(pl.multiple_of(t * 512, 512), 512)
        for e in range(2):
            fill(bpts.at[e], p_ref[:, pl.ds(pl.multiple_of(e * (n_pts // 2) + t * 512, 512), 512)], scale, False, cols)
        return 0

    with jax.named_scope("prep"):
        lax.fori_loop(0, n_cen // TILE, prep_own, 0)
        lax.fori_loop(0, n_pts // 1024, prep_pts, 0)

    part = n_cen // 8
    own_part = pl.ds(pl.multiple_of(d * part, part), part)

    def place(slab, pos):
        if slab in (0, 7):
            body, at_pos = slab, pos
        else:
            first = (slab + 1) // 2 * 2 - 1
            body, at_pos = first + pos // 2, 2 * (slab - first) + pos % 2
        return zbuf.at[body, :, at_pos * part : (at_pos + 1) * part]

    def a_z(slab):
        dest = at(d, ((z + (1 if slab % 2 else 7)) % 8) * 4 + x_lo * 2 + core)
        return remote(place(max(slab - 2, 0), 0), place(slab, 0), z_send.at[slab], z_recv.at[slab], dest)

    def a_x(slab):
        return remote(place(slab, 0), place(slab, 2), x_send.at[slab], x_recv.at[slab], x_next)

    def a_core(slab):
        return remote(place(slab, 0), place(slab, 1), c1_send.at[slab], c1_recv.at[slab], partner)

    def a_cross(slab):
        return remote(place(slab, 2), place(slab, 3), c3_send.at[slab], c3_recv.at[slab], partner)

    def z_came(slab):
        a_z(slab).wait_recv()
        if slab + 2 <= 7:
            a_z(slab + 2).start()
        a_core(slab).start()
        a_x(slab).start()

    def x_came(slab):
        a_x(slab).wait_recv()
        a_cross(slab).start()

    def arrived(body, h):
        if body in (0, 7):
            (a_cross if h else a_core)(body).wait_recv()
        else:
            slab = (body - 1) // 2 * 2 + 1 + h
            (a_core if body % 2 else a_cross)(slab).wait_recv()

    a_own = [
        pltpu.make_async_copy(src.at[:, own_part], zbuf.at[0, lo : lo + src.shape[0], 0:part], own_sem.at[n])
        for n, (src, lo) in enumerate(((c_ref, 0), (w_ref, feats)))
    ]
    for copy in a_own:
        copy.start()

    def nm_cols(t):
        return pl.ds(pl.multiple_of(t * WIDE, WIDE), WIDE)

    def nm_sum(t, ref):
        fpart[ref, :, nm_cols(t)] = dot(w_ref[...], kts[ref][:, nm_cols(t)])

    def nm_step(t, first):
        for ref in range(2):
            right = bpts[ref, :, nm_cols(t)]
            acc = None
            for b in range(n_cen // TILE):
                rows = pl.ds(b * TILE, TILE)
                if ref or not first:
                    one = dot(w_ref[:, rows], kts[1 - ref][rows, nm_cols(t + ref - 1)])
                    acc = one if acc is None else acc + one
                kts[ref][rows, nm_cols(t)] = jnp.exp2(dot(arow[rows, :], right)).astype(BF16)
            if ref or not first:
                fpart[1 - ref, :, nm_cols(t + ref - 1)] = acc

    piece = cpts // 2

    def d1(q):
        return remote(sbuf.at[q], dbuf.at[q], d1_send.at[q], d1_recv.at[q], partner)

    def d1_go(q):
        for e in range(2):
            sbuf[q, :, e * piece : (e + 1) * piece] = fpart[e, pl.ds(r_other, half), q * piece : (q + 1) * piece].astype(BF16)
        d1(q).start()

    def rs(q, k):
        lanes = pl.ds(pl.multiple_of(chip_peer(k) * share, share), share)
        return remote(rsend.at[q, :, lanes], rrecv.at[q, k], rs_send.at[q, k], rs_recv.at[q, k], group(k))

    own_rows = pl.ds(r_own, half)

    def rs_go(q):
        d1(q).wait_recv()
        for e in range(2):
            lanes = slice(e * piece, (e + 1) * piece)
            mine = fpart[e, own_rows, q * piece : (q + 1) * piece]
            rsend[q, :, lanes] = (mine + dbuf[q, :, lanes].astype(F32)).astype(BF16)
        for k in range(1, 16):
            rs(q, k).start()

    def own_share(q):
        return (chip // 8, own_rows, pl.ds(pl.multiple_of(q * piece + (chip % 8) * share, share), share))

    def ag(q, k):
        where = fwd.at[own_share(q)]
        return remote(where, where, ag_send.at[q, k], ag_recv.at[q, k], group(k))

    def ag_go(q):
        total = rsend[q, :, pl.ds(pl.multiple_of(chip * share, share), share)].astype(F32)
        for k in range(1, 16):
            rs(q, k).wait_recv()
            total = total + rrecv[q, k].astype(F32)
        fwd[own_share(q)] = total.astype(BF16)
        for k in range(1, 16):
            ag(q, k).start()

    def d2(q):
        where = fwd.at[:, own_rows, q * piece : (q + 1) * piece]
        return remote(where, where, d2_send.at[q], d2_recv.at[q], partner)

    def d2_go(q):
        for k in range(1, 16):
            ag(q, k).wait_recv()
        d2(q).start()

    hcen = n_cen // 2

    def mm_sum(body, ref, b, acc):
        rows = pl.ds(b * TILE, TILE)
        one = dot(zbuf[body, feats : feats + outs, rows], tiles[ref][rows, :])
        return one if acc is None else acc + one

    def mm_add(ref, acc, first):
        cols = slice(ref * hcen, (ref + 1) * hcen)
        mmacc[:, cols] = acc if first else mmacc[:, cols] + acc

    def mm(body, first):
        for h in range(2):
            cols = slice(h * WIDE, (h + 1) * WIDE)
            fill(zaug, zbuf[body, 0:feats, cols], scale, False, cols)
        for ref in range(2):
            acc = None
            for b in range(hcen // TILE):
                rows = pl.ds(b * TILE, TILE)
                if ref or not first:
                    acc = mm_sum(body + ref - 1, 1 - ref, b, acc)
                tiles[ref][rows, :] = jnp.exp2(dot(zaug[:, rows].T, bown[:, ref * hcen : (ref + 1) * hcen])).astype(BF16)
            if ref or not first:
                mm_add(1 - ref, acc, first)

    def actions(n, table):
        for step, todo in table.items():

            @pl.when(n == step)
            def _():
                for f, q in todo:
                    f(q)

    steps = n_pts // WIDE // 2
    with jax.named_scope("nm_a"):
        nm_step(0, True)
    with jax.named_scope("barrier"):
        pl.semaphore_wait(barrier, 23)
    for copy in a_own:
        copy.wait()
    a_z(1).start()
    a_z(2).start()
    a_x(0).start()
    a_core(0).start()

    def nm_body(n, _):
        with jax.named_scope("nm_body"):
            nm_step(n, False)
        with jax.named_scope("nm_act"):
            actions(n, {2: [(d1_go, 0), (z_came, 1), (z_came, 2), (x_came, 0)]})
        return 0

    lax.fori_loop(1, steps, nm_body, 0)
    with jax.named_scope("nm_end"):
        nm_sum(steps - 1, 1)
    with jax.named_scope("nm_end_act"):
        d1_go(1)
        rs_go(0)
        arrived(0, 0)
        arrived(0, 1)

    mmacc[:, hcen:] = jnp.zeros((outs, hcen), F32)
    with jax.named_scope("mm_0"):
        mm(0, True)
    with jax.named_scope("mm_0_act"):
        rs_go(1)
        z_came(3)
        z_came(4)
        x_came(1)
        x_came(2)
        arrived(1, 0)
        arrived(1, 1)

    table = {
        1: [],
        2: [(z_came, 5), (z_came, 6)],
        3: [(x_came, 3), (x_came, 4), (ag_go, 0)],
        4: [(z_came, 7)],
        5: [(x_came, 5), (x_came, 6), (ag_go, 1), (d2_go, 0)],
        6: [(x_came, 7), (d2_go, 1)],
    }

    def mm_body(n, _):
        with jax.named_scope("mm_body"):
            mm(n, False)
        with jax.named_scope("mm_act"):
            for step, todo in table.items():

                @pl.when(n == step)
                def _():
                    for f, q in todo:
                        f(q)
                    arrived(step + 1, 0)
                    arrived(step + 1, 1)

        return 0

    lax.fori_loop(1, 8, mm_body, 0)
    with jax.named_scope("mm_end"):
        acc = None
        for b in range(hcen // TILE):
            acc = mm_sum(7, 1, b, acc)
        mm_add(1, acc, False)
    with jax.named_scope("d2_wait"):
        d2(0).wait_recv()
        d2(1).wait_recv()

    hshare = dshare // 2

    def slice_of(peer, h):
        return pl.ds(pl.multiple_of(peer * dshare + h * hshare, hshare), hshare)

    def back(k, h):
        rows = slice_of(dp_peer(k), h)
        total = dot_nt(fwd[0], kta[rows, :]) + dot_nt(fwd[1], ktb[rows, :])
        return total * norm + mmacc[:, rows]

    def ds_copy(k, h):
        return remote(dsend.at[k, h], drecv.at[k, h], ds_send.at[k, h], ds_recv.at[k, h], at(dp_peer(k), c))

    def dg(k, h):
        where = outt.at[:, slice_of(d, h)]
        return remote(where, where, dg_send.at[k, h], dg_recv.at[k, h], at(dp_peer(k), c))

    def back_half(h):
        def step(k, _):
            dsend[k, h] = back(k, h)
            ds_copy(k, h).start()
            return 0

        lax.fori_loop(1, 8, step, 0)
        dsend[0, h] = back(0, h)

    def share_out(h):
        total = dsend[0, h]
        for k in range(1, 8):
            ds_copy(k, h).wait_recv()
            total = total + drecv[k, h]
        outt[:, slice_of(d, h)] = total
        for k in range(1, 8):
            dg(k, h).start()

    for h in range(2):
        with jax.named_scope(f"back_{h}"):
            back_half(h)
    for h in range(2):
        with jax.named_scope(f"share_{h}"):
            share_out(h)

    for slab in range(8):
        if slab:
            a_z(slab).wait_send()
        a_x(slab).wait_send()
        a_core(slab).wait_send()
        a_cross(slab).wait_send()
    for q in range(CHUNKS):
        d1(q).wait_send()
        d2(q).wait_send()
        for k in range(1, 16):
            rs(q, k).wait_send()
            ag(q, k).wait_send()
    for h in range(2):
        for k in range(1, 8):
            ds_copy(k, h).wait_send()
            with jax.named_scope(f"dg_{h}_{k}"):
                dg(k, h).wait_recv()
    with jax.named_scope("out"):
        out_ref[...] = outt[...]
    for h in range(2):
        for k in range(1, 8):
            dg(k, h).wait_send()


def solution(mesh):
    def on_device(points, centers, coef):
        n_pts, feats = points.shape
        n_cen, outs = coef.shape
        cpts = n_pts // CHUNKS
        dma = pltpu.SemaphoreType.DMA

        def body(*refs):
            kernel(feats, outs, n_pts, n_cen, n_pts * 8, *refs)

        return pl.pallas_call(
            body,
            out_shape=jax.ShapeDtypeStruct((outs, n_cen), F32),
            in_specs=[pl.BlockSpec(memory_space=pltpu.VMEM)] * 3,
            out_specs=pl.BlockSpec(memory_space=pltpu.VMEM),
            scratch_shapes=[
                pltpu.VMEM((2, ROWS, n_pts // 2), BF16),
                pltpu.VMEM((ROWS, n_cen), BF16),
                pltpu.VMEM((n_cen, ROWS), BF16),
                pltpu.VMEM((n_cen, n_pts // 2), BF16),
                pltpu.VMEM((n_cen, n_pts // 2), BF16),
                pltpu.VMEM((n_cen // 2, n_cen // 2), BF16),
                pltpu.VMEM((n_cen // 2, n_cen // 2), BF16),
                pltpu.VMEM((2, outs, n_pts // 2), F32),
                pltpu.VMEM((8, feats + outs, n_cen // 2), BF16),
                pltpu.VMEM((ROWS, n_cen // 2), BF16),
                pltpu.VMEM((outs, n_cen), F32),
                pltpu.VMEM((2, outs, n_pts // 2), BF16),
                pltpu.VMEM((CHUNKS, outs // 2, cpts), BF16),
                pltpu.VMEM((CHUNKS, outs // 2, cpts), BF16),
                pltpu.VMEM((CHUNKS, outs // 2, cpts), BF16),
                pltpu.VMEM((CHUNKS, 16, outs // 2, cpts // 16), BF16),
                pltpu.VMEM((8, 2, outs, n_cen // 16), F32),
                pltpu.VMEM((8, 2, outs, n_cen // 16), F32),
                pltpu.VMEM((outs, n_cen), F32),
                *[dma((8,))] * 8, dma((2,)),
                dma((CHUNKS,)), dma((CHUNKS,)),
                dma((CHUNKS, 16)), dma((CHUNKS, 16)),
                dma((CHUNKS, 16)), dma((CHUNKS, 16)),
                dma((CHUNKS,)), dma((CHUNKS,)),
                dma((8, 2)), dma((8, 2)),
                dma((8, 2)), dma((8, 2)),
            ],
            compiler_params=pltpu.CompilerParams(
                collective_id=0, has_side_effects=True, vmem_limit_bytes=60 * 1024 * 1024
            ),
        )(points.T, centers.T, coef.T).T

    in_specs = (P("dp", None), P("centers", None), P("centers", None))
    return jax.shard_map(
        on_device, mesh=mesh, in_specs=in_specs, out_specs=P("centers", None), check_vma=False
    )
```

```python
import math

import jax
import jax.numpy as jnp
import numpy as np
from jax import lax
from jax.experimental import pallas as pl
from jax.experimental.pallas import tpu as pltpu
from jax.sharding import PartitionSpec as P

F32, BF16 = jnp.float32, jnp.bfloat16
MESH = pl.DeviceIdType.MESH
ROWS = 128
TILE = 256
WIDE = 512
CHUNKS = 2


def split3(x):
    a = x.astype(BF16)
    r = x - a.astype(F32)
    b = r.astype(BF16)
    return a, b, (r - b.astype(F32)).astype(BF16)


def tail_rows(pieces, first, ones):
    n = pieces[0].shape[1]
    row = lax.broadcasted_iota(jnp.int32, (32, n), 0)
    out = jnp.where((row >= ones) & (row < ones + 3), 1.0, 0.0)
    for k, piece in enumerate(pieces):
        out = jnp.where(row == first + k, piece.astype(F32), out)
    return out.astype(BF16)


def fill(dst, feats, scale, scaled, cols):
    wide = feats.astype(F32)
    squares = split3(-scale * jnp.sum(wide * wide, axis=0, keepdims=True))
    parts = split3((2.0 * scale) * wide) if scaled else (feats,) * 3
    for k in range(3):
        dst[32 * k : 32 * (k + 1), cols] = parts[k]
    dst[96:128, cols] = tail_rows(squares, 3 if scaled else 0, 0 if scaled else 3)


def dot(a, b):
    return jnp.dot(a, b, preferred_element_type=F32)


def dot_nt(a, b):
    return lax.dot_general(a, b, (((1,), (1,)), ((), ())), preferred_element_type=F32)


def kernel(
    feats, outs, n_pts, n_cen, total_pts,
    p_ref, c_ref, w_ref, out_ref,
    bpts, bown, arow, kta, ktb, tilea, tileb, fpart, zbuf, zaug, zrow, mmacc, fwd,
    sbuf, dbuf, rsend, rrecv, dsend, drecv, outt,
    z_send, z_recv, x_send, x_recv, c1_send, c1_recv, c3_send, c3_recv, own_sem,
    d1_send, d1_recv, rs_send, rs_recv, ag_send, ag_recv,
    d2_send, d2_recv, ds_send, ds_recv, dg_send, dg_recv,
):
    scale = math.log2(math.e) * 2.0 / feats
    norm = float(np.float32(1.0) / np.sqrt(np.float32(total_pts)))
    d, c = lax.axis_index("dp"), lax.axis_index("centers")
    core, x_lo, z = c % 2, (c // 2) % 2, c // 4
    chip = c // 2
    y, x_hi = d // 2, d % 2
    kts, tiles = (kta, ktb), (tilea, tileb)
    half = outs // 2
    r_own = pl.multiple_of(half * core, half)
    r_other = pl.multiple_of(half * (1 - core), half)
    cpts = n_pts // CHUNKS
    share = cpts // 16
    dshare = n_cen // 8

    def at(dp, cen):
        return {"dp": dp, "centers": cen}

    partner = at(d, chip * 2 + 1 - core)
    x_next = at(d, z * 4 + (1 - x_lo) * 2 + core)

    def chip_peer(k):
        return (chip + k) % 16

    def group(k):
        return at(d, chip_peer(k) * 2 + core)

    def dp_peer(k):
        return (d + k) % 8

    def remote(src, dst, send, recv, dev):
        return pltpu.make_async_remote_copy(
            src_ref=src, dst_ref=dst, send_sem=send, recv_sem=recv, device_id=dev, device_id_type=MESH
        )

    barrier = pltpu.get_barrier_semaphore()
    for k in range(1, 16):
        pl.semaphore_signal(barrier, inc=1, device_id=group(k), device_id_type=MESH)
    pl.semaphore_signal(barrier, inc=1, device_id=partner, device_id_type=MESH)
    for k in range(1, 8):
        pl.semaphore_signal(barrier, inc=1, device_id=at(dp_peer(k), c), device_id_type=MESH)

    def prep_own(t, _):
        cols = pl.ds(pl.multiple_of(t * TILE, TILE), TILE)
        fill(bown, c_ref[:, cols], scale, True, cols)
        arow[cols, :] = bown[:, cols].T
        return 0

    def prep_pts(t, _):
        cols = pl.ds(pl.multiple_of(t * 512, 512), 512)
        for e in range(2):
            fill(bpts.at[e], p_ref[:, pl.ds(pl.multiple_of(e * (n_pts // 2) + t * 512, 512), 512)], scale, False, cols)
        return 0

    with jax.named_scope("prep"):
        lax.fori_loop(0, n_cen // TILE, prep_own, 0)
        lax.fori_loop(0, n_pts // 1024, prep_pts, 0)

    part = n_cen // 8
    own_part = pl.ds(pl.multiple_of(d * part, part), part)

    def place(slab, pos):
        if slab in (0, 7):
            body, at_pos = slab, pos
        else:
            first = (slab + 1) // 2 * 2 - 1
            body, at_pos = first + pos // 2, 2 * (slab - first) + pos % 2
        return zbuf.at[body, :, at_pos * part : (at_pos + 1) * part]

    def a_z(slab):
        dest = at(d, ((z + (1 if slab % 2 else 7)) % 8) * 4 + x_lo * 2 + core)
        return remote(place(max(slab - 2, 0), 0), place(slab, 0), z_send.at[slab], z_recv.at[slab], dest)

    def a_x(slab):
        return remote(place(slab, 0), place(slab, 2), x_send.at[slab], x_recv.at[slab], x_next)

    def a_core(slab):
        return remote(place(slab, 0), place(slab, 1), c1_send.at[slab], c1_recv.at[slab], partner)

    def a_cross(slab):
        return remote(place(slab, 2), place(slab, 3), c3_send.at[slab], c3_recv.at[slab], partner)

    def z_came(slab):
        a_z(slab).wait_recv()
        if slab + 2 <= 7:
            a_z(slab + 2).start()
        a_core(slab).start()
        a_x(slab).start()

    def x_came(slab):
        a_x(slab).wait_recv()
        a_cross(slab).start()

    def arrived(body, h):
        if body in (0, 7):
            (a_cross if h else a_core)(body).wait_recv()
        else:
            slab = (body - 1) // 2 * 2 + 1 + h
            (a_core if body % 2 else a_cross)(slab).wait_recv()

    a_own = [
        pltpu.make_async_copy(src.at[:, own_part], zbuf.at[0, lo : lo + src.shape[0], 0:part], own_sem.at[n])
        for n, (src, lo) in enumerate(((c_ref, 0), (w_ref, feats)))
    ]
    for copy in a_own:
        copy.start()

    def nm_cols(t):
        return pl.ds(pl.multiple_of(t * WIDE, WIDE), WIDE)

    def nm_sum(t, ref):
        fpart[ref, :, nm_cols(t)] = dot(w_ref[...], kts[ref][:, nm_cols(t)])

    def nm_step(t, first):
        for ref in range(2):
            right = bpts[ref, :, nm_cols(t)]
            acc = None
            for b in range(n_cen // TILE):
                rows = pl.ds(b * TILE, TILE)
                if ref or not first:
                    one = dot(w_ref[:, rows], kts[1 - ref][rows, nm_cols(t + ref - 1)])
                    acc = one if acc is None else acc + one
                kts[ref][rows, nm_cols(t)] = jnp.exp2(dot(arow[rows, :], right)).astype(BF16)
            if ref or not first:
                fpart[1 - ref, :, nm_cols(t + ref - 1)] = acc

    piece = cpts // 2

    def d1(q):
        return remote(sbuf.at[q], dbuf.at[q], d1_send.at[q], d1_recv.at[q], partner)

    def d1_go(q):
        for e in range(2):
            sbuf[q, :, e * piece : (e + 1) * piece] = fpart[e, pl.ds(r_other, half), q * piece : (q + 1) * piece].astype(BF16)
        d1(q).start()

    def rs(q, k):
        lanes = pl.ds(pl.multiple_of(chip_peer(k) * share, share), share)
        return remote(rsend.at[q, :, lanes], rrecv.at[q, k], rs_send.at[q, k], rs_recv.at[q, k], group(k))

    own_rows = pl.ds(r_own, half)

    def rs_go(q):
        d1(q).wait_recv()
        for e in range(2):
            lanes = slice(e * piece, (e + 1) * piece)
            mine = fpart[e, own_rows, q * piece : (q + 1) * piece]
            rsend[q, :, lanes] = (mine + dbuf[q, :, lanes].astype(F32)).astype(BF16)
        for k in range(1, 16):
            rs(q, k).start()

    def own_share(q):
        return (chip // 8, own_rows, pl.ds(pl.multiple_of(q * piece + (chip % 8) * share, share), share))

    def ag(q, k):
        where = fwd.at[own_share(q)]
        return remote(where, where, ag_send.at[q, k], ag_recv.at[q, k], group(k))

    def ag_go(q):
        total = rsend[q, :, pl.ds(pl.multiple_of(chip * share, share), share)].astype(F32)
        for k in range(1, 16):
            rs(q, k).wait_recv()
            total = total + rrecv[q, k].astype(F32)
        fwd[own_share(q)] = total.astype(BF16)
        for k in range(1, 16):
            ag(q, k).start()

    def d2(q):
        where = fwd.at[:, own_rows, q * piece : (q + 1) * piece]
        return remote(where, where, d2_send.at[q], d2_recv.at[q], partner)

    def d2_go(q):
        for k in range(1, 16):
            ag(q, k).wait_recv()
        d2(q).start()

    hcen = n_cen // 2

    def mm_sum(body, ref, b, acc):
        rows = pl.ds(b * TILE, TILE)
        one = dot(zbuf[body, feats : feats + outs, rows], tiles[ref][rows, :])
        return one if acc is None else acc + one

    def mm_add(ref, acc, first):
        cols = slice(ref * hcen, (ref + 1) * hcen)
        mmacc[:, cols] = acc if first else mmacc[:, cols] + acc

    def mm(body, first):
        for h in range(2):
            cols = slice(h * WIDE, (h + 1) * WIDE)
            fill(zaug, zbuf[body, 0:feats, cols], scale, False, cols)
            zrow[cols, :] = zaug[:, cols].T
        for ref in range(2):
            acc = None
            for b in range(hcen // TILE):
                rows = pl.ds(b * TILE, TILE)
                if ref or not first:
                    acc = mm_sum(body + ref - 1, 1 - ref, b, acc)
                tiles[ref][rows, :] = jnp.exp2(dot(zrow[rows, :], bown[:, ref * hcen : (ref + 1) * hcen])).astype(BF16)
            if ref or not first:
                mm_add(1 - ref, acc, first)

    def actions(n, table):
        for step, todo in table.items():

            @pl.when(n == step)
            def _():
                for f, q in todo:
                    f(q)

    steps = n_pts // WIDE // 2
    with jax.named_scope("nm_a"):
        nm_step(0, True)
    with jax.named_scope("barrier"):
        pl.semaphore_wait(barrier, 23)
    for copy in a_own:
        copy.wait()
    a_z(1).start()
    a_z(2).start()
    a_x(0).start()
    a_core(0).start()

    def nm_body(n, _):
        with jax.named_scope("nm_body"):
            nm_step(n, False)
        with jax.named_scope("nm_act"):
            actions(n, {2: [(d1_go, 0), (z_came, 1), (z_came, 2), (x_came, 0)]})
        return 0

    lax.fori_loop(1, steps, nm_body, 0)
    with jax.named_scope("nm_end"):
        nm_sum(steps - 1, 1)
    with jax.named_scope("nm_end_act"):
        d1_go(1)
        rs_go(0)
        arrived(0, 0)
        arrived(0, 1)

    mmacc[:, hcen:] = jnp.zeros((outs, hcen), F32)
    with jax.named_scope("mm_0"):
        mm(0, True)
    with jax.named_scope("mm_0_act"):
        z_came(3)
        z_came(4)
        rs_go(1)
        x_came(1)
        x_came(2)
        arrived(1, 0)
        arrived(1, 1)

    table = {
        1: [],
        2: [(z_came, 5), (z_came, 6)],
        3: [(x_came, 3), (x_came, 4), (ag_go, 0)],
        4: [(z_came, 7), (ag_go, 1)],
        5: [(x_came, 5), (x_came, 6)],
        6: [(x_came, 7), (d2_go, 0)],
    }

    def mm_body(n, _):
        with jax.named_scope("mm_body"):
            mm(n, False)
        with jax.named_scope("mm_act"):
            for step, todo in table.items():

                @pl.when(n == step)
                def _():
                    for f, q in todo:
                        f(q)
                    arrived(step + 1, 0)
                    arrived(step + 1, 1)

        return 0

    lax.fori_loop(1, 8, mm_body, 0)
    with jax.named_scope("d2_1"):
        d2_go(1)
    with jax.named_scope("mm_end"):
        acc = None
        for b in range(hcen // TILE):
            acc = mm_sum(7, 1, b, acc)
        mm_add(1, acc, False)
    with jax.named_scope("d2_wait"):
        d2(0).wait_recv()
        d2(1).wait_recv()

    hshare = dshare // 2

    def slice_of(peer, h):
        return pl.ds(pl.multiple_of(peer * dshare + h * hshare, hshare), hshare)

    def back(k, h):
        rows = slice_of(dp_peer(k), h)
        total = dot_nt(fwd[0], kta[rows, :]) + dot_nt(fwd[1], ktb[rows, :])
        return total * norm + mmacc[:, rows]

    def ds_copy(k, h):
        return remote(dsend.at[k, h], drecv.at[k, h], ds_send.at[k, h], ds_recv.at[k, h], at(dp_peer(k), c))

    def dg(k, h):
        where = outt.at[:, slice_of(d, h)]
        return remote(where, where, dg_send.at[k, h], dg_recv.at[k, h], at(dp_peer(k), c))

    def back_half(h):
        def step(t, _):
            for k in (2 * t + 1, 2 * t + 2):
                dsend[k % 8, h] = back(k, h)
            ds_copy(2 * t + 1, h).start()

            @pl.when(t < 3)
            def _():
                ds_copy(2 * t + 2, h).start()

            return 0

        lax.fori_loop(0, 4, step, 0)

    def share_out(h):
        total = dsend[0, h]
        for k in range(1, 8):
            ds_copy(k, h).wait_recv()
            total = total + drecv[k, h]
        outt[:, slice_of(d, h)] = total
        for k in range(1, 8):
            dg(k, h).start()

    for h in range(2):
        with jax.named_scope(f"back_{h}"):
            back_half(h)
    for h in range(2):
        with jax.named_scope(f"share_{h}"):
            share_out(h)

    for slab in range(8):
        if slab:
            a_z(slab).wait_send()
        a_x(slab).wait_send()
        a_core(slab).wait_send()
        a_cross(slab).wait_send()
    for q in range(CHUNKS):
        d1(q).wait_send()
        d2(q).wait_send()
        for k in range(1, 16):
            rs(q, k).wait_send()
            ag(q, k).wait_send()
    for h in range(2):
        for k in range(1, 8):
            ds_copy(k, h).wait_send()
            with jax.named_scope(f"dg_{h}_{k}"):
                dg(k, h).wait_recv()
    with jax.named_scope("out"):
        out_ref[...] = outt[...]
    for h in range(2):
        for k in range(1, 8):
            dg(k, h).wait_send()


def solution(mesh):
    def on_device(points, centers, coef):
        n_pts, feats = points.shape
        n_cen, outs = coef.shape
        cpts = n_pts // CHUNKS
        dma = pltpu.SemaphoreType.DMA

        def body(*refs):
            kernel(feats, outs, n_pts, n_cen, n_pts * 8, *refs)

        return pl.pallas_call(
            body,
            out_shape=jax.ShapeDtypeStruct((outs, n_cen), F32),
            in_specs=[pl.BlockSpec(memory_space=pltpu.VMEM)] * 3,
            out_specs=pl.BlockSpec(memory_space=pltpu.VMEM),
            scratch_shapes=[
                pltpu.VMEM((2, ROWS, n_pts // 2), BF16),
                pltpu.VMEM((ROWS, n_cen), BF16),
                pltpu.VMEM((n_cen, ROWS), BF16),
                pltpu.VMEM((n_cen, n_pts // 2), BF16),
                pltpu.VMEM((n_cen, n_pts // 2), BF16),
                pltpu.VMEM((n_cen // 2, n_cen // 2), BF16),
                pltpu.VMEM((n_cen // 2, n_cen // 2), BF16),
                pltpu.VMEM((2, outs, n_pts // 2), F32),
                pltpu.VMEM((8, feats + outs, n_cen // 2), BF16),
                pltpu.VMEM((ROWS, n_cen // 2), BF16),
                pltpu.VMEM((n_cen // 2, ROWS), BF16),
                pltpu.VMEM((outs, n_cen), F32),
                pltpu.VMEM((2, outs, n_pts // 2), BF16),
                pltpu.VMEM((CHUNKS, outs // 2, cpts), BF16),
                pltpu.VMEM((CHUNKS, outs // 2, cpts), BF16),
                pltpu.VMEM((CHUNKS, outs // 2, cpts), BF16),
                pltpu.VMEM((CHUNKS, 16, outs // 2, cpts // 16), BF16),
                pltpu.VMEM((8, 2, outs, n_cen // 16), F32),
                pltpu.VMEM((8, 2, outs, n_cen // 16), F32),
                pltpu.VMEM((outs, n_cen), F32),
                *[dma((8,))] * 8, dma((2,)),
                dma((CHUNKS,)), dma((CHUNKS,)),
                dma((CHUNKS, 16)), dma((CHUNKS, 16)),
                dma((CHUNKS, 16)), dma((CHUNKS, 16)),
                dma((CHUNKS,)), dma((CHUNKS,)),
                dma((8, 2)), dma((8, 2)),
                dma((8, 2)), dma((8, 2)),
            ],
            compiler_params=pltpu.CompilerParams(
                collective_id=0, has_side_effects=True, vmem_limit_bytes=40 * 1024 * 1024
            ),
        )(points.T, centers.T, coef.T).T

    in_specs = (P("dp", None), P("centers", None), P("centers", None))
    return jax.shard_map(
        on_device, mesh=mesh, in_specs=in_specs, out_specs=P("centers", None), check_vma=False
    )
```

```python
import math

import jax
import jax.numpy as jnp
import numpy as np
from jax import lax
from jax.experimental import pallas as pl
from jax.experimental.pallas import tpu as pltpu
from jax.sharding import PartitionSpec as P

F32, BF16 = jnp.float32, jnp.bfloat16
MESH = pl.DeviceIdType.MESH
ROWS = 128
TILE = 256
WIDE = 512
CHUNKS = 2


def split3(x):
    a = x.astype(BF16)
    r = x - a.astype(F32)
    b = r.astype(BF16)
    return a, b, (r - b.astype(F32)).astype(BF16)


def tail_rows(pieces, first, ones):
    n = pieces[0].shape[1]
    row = lax.broadcasted_iota(jnp.int32, (32, n), 0)
    out = jnp.where((row >= ones) & (row < ones + 3), 1.0, 0.0)
    for k, piece in enumerate(pieces):
        out = jnp.where(row == first + k, piece.astype(F32), out)
    return out.astype(BF16)


def fill(dst, feats, scale, scaled, cols):
    wide = feats.astype(F32)
    squares = split3(-scale * jnp.sum(wide * wide, axis=0, keepdims=True))
    parts = split3((2.0 * scale) * wide) if scaled else (feats,) * 3
    for k in range(3):
        dst[32 * k : 32 * (k + 1), cols] = parts[k]
    dst[96:128, cols] = tail_rows(squares, 3 if scaled else 0, 0 if scaled else 3)


def dot(a, b):
    return jnp.dot(a, b, preferred_element_type=F32)


def dot_nt(a, b):
    return lax.dot_general(a, b, (((1,), (1,)), ((), ())), preferred_element_type=F32)


def kernel(
    feats, outs, n_pts, n_cen, total_pts,
    p_hbm, c_hbm, w_hbm, out_ref,
    p_ref, c_ref, w_ref,
    bpts, bown, arow, kta, ktb, tilea, tileb, fpart, zbuf, zaug, zrow, mmacc, fwd,
    sbuf, dbuf, rsend, rrecv, dsend, drecv, outt,
    z_send, z_recv, x_send, x_recv, c1_send, c1_recv, c3_send, c3_recv, own_sem, in_sem,
    d1_send, d1_recv, rs_send, rs_recv, ag_send, ag_recv,
    d2_send, d2_recv, ds_send, ds_recv, dg_send, dg_recv,
):
    scale = math.log2(math.e) * 2.0 / feats
    norm = float(np.float32(1.0) / np.sqrt(np.float32(total_pts)))
    d, c = lax.axis_index("dp"), lax.axis_index("centers")
    core, x_lo, z = c % 2, (c // 2) % 2, c // 4
    chip = c // 2
    y, x_hi = d // 2, d % 2
    kts, tiles = (kta, ktb), (tilea, tileb)
    half = outs // 2
    r_own = pl.multiple_of(half * core, half)
    r_other = pl.multiple_of(half * (1 - core), half)
    cpts = n_pts // CHUNKS
    share = cpts // 16
    dshare = n_cen // 8

    def at(dp, cen):
        return {"dp": dp, "centers": cen}

    partner = at(d, chip * 2 + 1 - core)
    x_next = at(d, z * 4 + (1 - x_lo) * 2 + core)

    def chip_peer(k):
        return (chip + k) % 16

    def group(k):
        return at(d, chip_peer(k) * 2 + core)

    def dp_peer(k):
        return (d + k) % 8

    def remote(src, dst, send, recv, dev):
        return pltpu.make_async_remote_copy(
            src_ref=src, dst_ref=dst, send_sem=send, recv_sem=recv, device_id=dev, device_id_type=MESH
        )

    fetch = [
        pltpu.make_async_copy(src, dst, in_sem.at[n])
        for n, (src, dst) in enumerate(((c_hbm, c_ref), (p_hbm, p_ref), (w_hbm, w_ref)))
    ]
    for copy in fetch:
        copy.start()

    barrier = pltpu.get_barrier_semaphore()
    for k in range(1, 16):
        pl.semaphore_signal(barrier, inc=1, device_id=group(k), device_id_type=MESH)
    pl.semaphore_signal(barrier, inc=1, device_id=partner, device_id_type=MESH)
    for k in range(1, 8):
        pl.semaphore_signal(barrier, inc=1, device_id=at(dp_peer(k), c), device_id_type=MESH)

    def prep_own(t, _):
        cols = pl.ds(pl.multiple_of(t * TILE, TILE), TILE)
        fill(bown, c_ref[:, cols], scale, True, cols)
        arow[cols, :] = bown[:, cols].T
        return 0

    def prep_pts(t, _):
        cols = pl.ds(pl.multiple_of(t * 512, 512), 512)
        for e in range(2):
            fill(bpts.at[e], p_ref[:, pl.ds(pl.multiple_of(e * (n_pts // 2) + t * 512, 512), 512)], scale, False, cols)
        return 0

    with jax.named_scope("prep"):
        fetch[0].wait()
        lax.fori_loop(0, n_cen // TILE, prep_own, 0)
        fetch[1].wait()
        lax.fori_loop(0, n_pts // 1024, prep_pts, 0)

    part = n_cen // 8
    own_part = pl.ds(pl.multiple_of(d * part, part), part)

    def place(slab, pos):
        if slab in (0, 7):
            body, at_pos = slab, pos
        else:
            first = (slab + 1) // 2 * 2 - 1
            body, at_pos = first + pos // 2, 2 * (slab - first) + pos % 2
        return zbuf.at[body, :, at_pos * part : (at_pos + 1) * part]

    def a_z(slab):
        dest = at(d, ((z + (1 if slab % 2 else 7)) % 8) * 4 + x_lo * 2 + core)
        return remote(place(max(slab - 2, 0), 0), place(slab, 0), z_send.at[slab], z_recv.at[slab], dest)

    def a_x(slab):
        return remote(place(slab, 0), place(slab, 2), x_send.at[slab], x_recv.at[slab], x_next)

    def a_core(slab):
        return remote(place(slab, 0), place(slab, 1), c1_send.at[slab], c1_recv.at[slab], partner)

    def a_cross(slab):
        return remote(place(slab, 2), place(slab, 3), c3_send.at[slab], c3_recv.at[slab], partner)

    def z_came(slab):
        a_z(slab).wait_recv()
        if slab + 2 <= 7:
            a_z(slab + 2).start()
        a_core(slab).start()
        a_x(slab).start()

    def x_came(slab):
        a_x(slab).wait_recv()
        a_cross(slab).start()

    def arrived(body, h):
        if body in (0, 7):
            (a_cross if h else a_core)(body).wait_recv()
        else:
            slab = (body - 1) // 2 * 2 + 1 + h
            (a_core if body % 2 else a_cross)(slab).wait_recv()

    a_own = [
        pltpu.make_async_copy(src.at[:, own_part], zbuf.at[0, lo : lo + src.shape[0], 0:part], own_sem.at[n])
        for n, (src, lo) in enumerate(((c_hbm, 0), (w_hbm, feats)))
    ]
    for copy in a_own:
        copy.start()

    def nm_cols(t):
        return pl.ds(pl.multiple_of(t * WIDE, WIDE), WIDE)

    def nm_sum(t, ref):
        fpart[ref, :, nm_cols(t)] = dot(w_ref[...], kts[ref][:, nm_cols(t)])

    def nm_step(t, first):
        for ref in range(2):
            right = bpts[ref, :, nm_cols(t)]
            acc = None
            for b in range(n_cen // TILE):
                rows = pl.ds(b * TILE, TILE)
                if ref or not first:
                    one = dot(w_ref[:, rows], kts[1 - ref][rows, nm_cols(t + ref - 1)])
                    acc = one if acc is None else acc + one
                kts[ref][rows, nm_cols(t)] = jnp.exp2(dot(arow[rows, :], right)).astype(BF16)
            if ref or not first:
                fpart[1 - ref, :, nm_cols(t + ref - 1)] = acc

    piece = cpts // 2

    def d1(q):
        return remote(sbuf.at[q], dbuf.at[q], d1_send.at[q], d1_recv.at[q], partner)

    def d1_go(q):
        for e in range(2):
            sbuf[q, :, e * piece : (e + 1) * piece] = fpart[e, pl.ds(r_other, half), q * piece : (q + 1) * piece].astype(BF16)
        d1(q).start()

    def rs(q, k):
        lanes = pl.ds(pl.multiple_of(chip_peer(k) * share, share), share)
        return remote(rsend.at[q, :, lanes], rrecv.at[q, k], rs_send.at[q, k], rs_recv.at[q, k], group(k))

    own_rows = pl.ds(r_own, half)

    def rs_go(q):
        d1(q).wait_recv()
        for e in range(2):
            lanes = slice(e * piece, (e + 1) * piece)
            mine = fpart[e, own_rows, q * piece : (q + 1) * piece]
            rsend[q, :, lanes] = (mine + dbuf[q, :, lanes].astype(F32)).astype(BF16)
        for k in range(1, 16):
            rs(q, k).start()

    def own_share(q):
        return (chip // 8, own_rows, pl.ds(pl.multiple_of(q * piece + (chip % 8) * share, share), share))

    def ag(q, k):
        where = fwd.at[own_share(q)]
        return remote(where, where, ag_send.at[q, k], ag_recv.at[q, k], group(k))

    def ag_go(q):
        total = rsend[q, :, pl.ds(pl.multiple_of(chip * share, share), share)].astype(F32)
        for k in range(1, 16):
            rs(q, k).wait_recv()
            total = total + rrecv[q, k].astype(F32)
        fwd[own_share(q)] = total.astype(BF16)
        for k in range(1, 16):
            ag(q, k).start()

    def d2(q):
        where = fwd.at[:, own_rows, q * piece : (q + 1) * piece]
        return remote(where, where, d2_send.at[q], d2_recv.at[q], partner)

    def d2_go(q):
        for k in range(1, 16):
            ag(q, k).wait_recv()
        d2(q).start()

    hcen = n_cen // 2

    def mm_sum(body, ref, b, acc):
        rows = pl.ds(b * TILE, TILE)
        one = dot(zbuf[body, feats : feats + outs, rows], tiles[ref][rows, :])
        return one if acc is None else acc + one

    def mm_add(ref, acc, first):
        cols = slice(ref * hcen, (ref + 1) * hcen)
        mmacc[:, cols] = acc if first else mmacc[:, cols] + acc

    def mm(body, first):
        for h in range(2):
            cols = slice(h * WIDE, (h + 1) * WIDE)
            fill(zaug, zbuf[body, 0:feats, cols], scale, False, cols)
            zrow[cols, :] = zaug[:, cols].T
        for ref in range(2):
            acc = None
            for b in range(hcen // TILE):
                rows = pl.ds(b * TILE, TILE)
                if ref or not first:
                    acc = mm_sum(body + ref - 1, 1 - ref, b, acc)
                tiles[ref][rows, :] = jnp.exp2(dot(zrow[rows, :], bown[:, ref * hcen : (ref + 1) * hcen])).astype(BF16)
            if ref or not first:
                mm_add(1 - ref, acc, first)

    def actions(n, table):
        for step, todo in table.items():

            @pl.when(n == step)
            def _():
                for f, q in todo:
                    f(q)

    steps = n_pts // WIDE // 2
    fetch[2].wait()
    with jax.named_scope("nm_a"):
        nm_step(0, True)
    with jax.named_scope("barrier"):
        pl.semaphore_wait(barrier, 23)
    for copy in a_own:
        copy.wait()
    a_z(1).start()
    a_z(2).start()
    a_x(0).start()
    a_core(0).start()

    def nm_body(n, _):
        with jax.named_scope("nm_body"):
            nm_step(n, False)
        with jax.named_scope("nm_act"):
            actions(n, {2: [(d1_go, 0), (z_came, 1), (z_came, 2), (x_came, 0)]})
        return 0

    lax.fori_loop(1, steps, nm_body, 0)
    with jax.named_scope("nm_end"):
        nm_sum(steps - 1, 1)
    with jax.named_scope("nm_end_act"):
        d1_go(1)
        rs_go(0)
        arrived(0, 0)
        arrived(0, 1)

    mmacc[:, hcen:] = jnp.zeros((outs, hcen), F32)
    with jax.named_scope("mm_0"):
        mm(0, True)
    with jax.named_scope("mm_0_act"):
        z_came(3)
        z_came(4)
        rs_go(1)
        x_came(1)
        x_came(2)
        arrived(1, 0)
        arrived(1, 1)

    table = {
        1: [],
        2: [(z_came, 5), (z_came, 6), (x_came, 3), (x_came, 4), (ag_go, 0)],
        3: [(ag_go, 1)],
        4: [(z_came, 7), (x_came, 5), (x_came, 6)],
        5: [(x_came, 7), (d2_go, 0)],
        6: [(d2_go, 1)],
    }

    def mm_body(n, _):
        with jax.named_scope("mm_body"):
            mm(n, False)
        with jax.named_scope("mm_act"):
            for step, todo in table.items():

                @pl.when(n == step)
                def _():
                    for f, q in todo:
                        with jax.named_scope(f"{f.__name__}_{q}"):
                            f(q)
                    with jax.named_scope(f"arrived_{step + 1}"):
                        arrived(step + 1, 0)
                        arrived(step + 1, 1)

        return 0

    lax.fori_loop(1, 8, mm_body, 0)
    with jax.named_scope("mm_end"):
        acc = None
        for b in range(hcen // TILE):
            acc = mm_sum(7, 1, b, acc)
        mm_add(1, acc, False)
    with jax.named_scope("d2_wait"):
        d2(0).wait_recv()
        d2(1).wait_recv()

    hshare = dshare // 2

    def slice_of(peer, h):
        return pl.ds(pl.multiple_of(peer * dshare + h * hshare, hshare), hshare)

    def back(k, h):
        rows = slice_of(dp_peer(k), h)
        total = dot_nt(fwd[0], kta[rows, :]) + dot_nt(fwd[1], ktb[rows, :])
        return total * norm + mmacc[:, rows]

    def ds_copy(k, h):
        return remote(dsend.at[k, h], drecv.at[k, h], ds_send.at[k, h], ds_recv.at[k, h], at(dp_peer(k), c))

    def dg(k, h):
        where = outt.at[:, slice_of(d, h)]
        return remote(where, where, dg_send.at[k, h], dg_recv.at[k, h], at(dp_peer(k), c))

    def back_half(h):
        def step(t, _):
            for k in (2 * t + 1, 2 * t + 2):
                dsend[k % 8, h] = back(k, h)
            ds_copy(2 * t + 1, h).start()

            @pl.when(t < 3)
            def _():
                ds_copy(2 * t + 2, h).start()

            return 0

        lax.fori_loop(0, 4, step, 0)

    def share_out(h):
        total = dsend[0, h]
        for k in range(1, 8):
            ds_copy(k, h).wait_recv()
            total = total + drecv[k, h]
        outt[:, slice_of(d, h)] = total
        for k in range(1, 8):
            dg(k, h).start()

    for h in range(2):
        with jax.named_scope(f"back_{h}"):
            back_half(h)
    for h in range(2):
        with jax.named_scope(f"share_{h}"):
            share_out(h)

    for slab in range(8):
        if slab:
            a_z(slab).wait_send()
        a_x(slab).wait_send()
        a_core(slab).wait_send()
        a_cross(slab).wait_send()
    for q in range(CHUNKS):
        d1(q).wait_send()
        d2(q).wait_send()
        for k in range(1, 16):
            rs(q, k).wait_send()
            ag(q, k).wait_send()
    for h in range(2):
        for k in range(1, 8):
            ds_copy(k, h).wait_send()
            with jax.named_scope(f"dg_{h}_{k}"):
                dg(k, h).wait_recv()
    with jax.named_scope("out"):
        out_ref[...] = outt[...]
    for h in range(2):
        for k in range(1, 8):
            dg(k, h).wait_send()


def solution(mesh):
    def on_device(points, centers, coef):
        n_pts, feats = points.shape
        n_cen, outs = coef.shape
        cpts = n_pts // CHUNKS
        dma = pltpu.SemaphoreType.DMA

        def body(*refs):
            kernel(feats, outs, n_pts, n_cen, n_pts * 8, *refs)

        return pl.pallas_call(
            body,
            out_shape=jax.ShapeDtypeStruct((outs, n_cen), F32),
            in_specs=[pl.BlockSpec(memory_space=pltpu.HBM)] * 3,
            out_specs=pl.BlockSpec(memory_space=pltpu.VMEM),
            scratch_shapes=[
                pltpu.VMEM((feats, n_pts), BF16),
                pltpu.VMEM((feats, n_cen), BF16),
                pltpu.VMEM((outs, n_cen), BF16),
                pltpu.VMEM((2, ROWS, n_pts // 2), BF16),
                pltpu.VMEM((ROWS, n_cen), BF16),
                pltpu.VMEM((n_cen, ROWS), BF16),
                pltpu.VMEM((n_cen, n_pts // 2), BF16),
                pltpu.VMEM((n_cen, n_pts // 2), BF16),
                pltpu.VMEM((n_cen // 2, n_cen // 2), BF16),
                pltpu.VMEM((n_cen // 2, n_cen // 2), BF16),
                pltpu.VMEM((2, outs, n_pts // 2), F32),
                pltpu.VMEM((8, feats + outs, n_cen // 2), BF16),
                pltpu.VMEM((ROWS, n_cen // 2), BF16),
                pltpu.VMEM((n_cen // 2, ROWS), BF16),
                pltpu.VMEM((outs, n_cen), F32),
                pltpu.VMEM((2, outs, n_pts // 2), BF16),
                pltpu.VMEM((CHUNKS, outs // 2, cpts), BF16),
                pltpu.VMEM((CHUNKS, outs // 2, cpts), BF16),
                pltpu.VMEM((CHUNKS, outs // 2, cpts), BF16),
                pltpu.VMEM((CHUNKS, 16, outs // 2, cpts // 16), BF16),
                pltpu.VMEM((8, 2, outs, n_cen // 16), F32),
                pltpu.VMEM((8, 2, outs, n_cen // 16), F32),
                pltpu.VMEM((outs, n_cen), F32),
                *[dma((8,))] * 8, dma((2,)), dma((3,)),
                dma((CHUNKS,)), dma((CHUNKS,)),
                dma((CHUNKS, 16)), dma((CHUNKS, 16)),
                dma((CHUNKS, 16)), dma((CHUNKS, 16)),
                dma((CHUNKS,)), dma((CHUNKS,)),
                dma((8, 2)), dma((8, 2)),
                dma((8, 2)), dma((8, 2)),
            ],
            compiler_params=pltpu.CompilerParams(
                collective_id=0, has_side_effects=True, vmem_limit_bytes=40 * 1024 * 1024
            ),
        )(*(pltpu.with_memory_space_constraint(a.T, pltpu.HBM) for a in (points, centers, coef))).T

    in_specs = (P("dp", None), P("centers", None), P("centers", None))
    return jax.shard_map(
        on_device, mesh=mesh, in_specs=in_specs, out_specs=P("centers", None), check_vma=False
    )
```

```python
import math

import jax
import jax.numpy as jnp
import numpy as np
from jax import lax
from jax.experimental import pallas as pl
from jax.experimental.pallas import tpu as pltpu
from jax.sharding import PartitionSpec as P

F32, BF16 = jnp.float32, jnp.bfloat16
MESH = pl.DeviceIdType.MESH
ROWS = 128
TILE = 256
WIDE = 512
CHUNKS = 2


def split3(x):
    a = x.astype(BF16)
    r = x - a.astype(F32)
    b = r.astype(BF16)
    return a, b, (r - b.astype(F32)).astype(BF16)


def tail_rows(pieces, first, ones):
    n = pieces[0].shape[1]
    row = lax.broadcasted_iota(jnp.int32, (32, n), 0)
    out = jnp.where((row >= ones) & (row < ones + 3), 1.0, 0.0)
    for k, piece in enumerate(pieces):
        out = jnp.where(row == first + k, piece.astype(F32), out)
    return out.astype(BF16)


def fill(dst, feats, scale, scaled, cols):
    wide = feats.astype(F32)
    squares = split3(-scale * jnp.sum(wide * wide, axis=0, keepdims=True))
    parts = split3((2.0 * scale) * wide) if scaled else (feats,) * 3
    for k in range(3):
        dst[32 * k : 32 * (k + 1), cols] = parts[k]
    dst[96:128, cols] = tail_rows(squares, 3 if scaled else 0, 0 if scaled else 3)


def dot(a, b):
    return jnp.dot(a, b, preferred_element_type=F32)


def dot_nt(a, b):
    return lax.dot_general(a, b, (((1,), (1,)), ((), ())), preferred_element_type=F32)


def kernel(
    feats, outs, n_pts, n_cen, total_pts,
    p_hbm, c_hbm, w_hbm, out_ref,
    p_ref, c_ref, w_ref,
    bpts, bown, arow, kta, ktb, tilea, tileb, fpart, zbuf, zaug, zrow, mmacc, fwd,
    sbuf, dbuf, rsend, rrecv, dsend, drecv, outt,
    z_send, z_recv, x_send, x_recv, c1_send, c1_recv, c3_send, c3_recv, own_sem, in_sem,
    d1_send, d1_recv, rs_send, rs_recv, ag_send, ag_recv,
    d2_send, d2_recv, ds_send, ds_recv, dg_send, dg_recv,
):
    scale = math.log2(math.e) * 2.0 / feats
    norm = float(np.float32(1.0) / np.sqrt(np.float32(total_pts)))
    d, c = lax.axis_index("dp"), lax.axis_index("centers")
    core, x_lo, z = c % 2, (c // 2) % 2, c // 4
    chip = c // 2
    y, x_hi = d // 2, d % 2
    kts, tiles = (kta, ktb), (tilea, tileb)
    half = outs // 2
    r_own = pl.multiple_of(half * core, half)
    r_other = pl.multiple_of(half * (1 - core), half)
    cpts = n_pts // CHUNKS
    share = cpts // 16
    dshare = n_cen // 8

    def at(dp, cen):
        return {"dp": dp, "centers": cen}

    partner = at(d, chip * 2 + 1 - core)
    x_next = at(d, z * 4 + (1 - x_lo) * 2 + core)
    x_cross = at(d, z * 4 + (1 - x_lo) * 2 + 1 - core)

    def chip_peer(k):
        return (chip + k) % 16

    def group(k):
        return at(d, chip_peer(k) * 2 + core)

    def dp_peer(k):
        return (d + k) % 8

    def remote(src, dst, send, recv, dev):
        return pltpu.make_async_remote_copy(
            src_ref=src, dst_ref=dst, send_sem=send, recv_sem=recv, device_id=dev, device_id_type=MESH
        )

    fetch = [
        pltpu.make_async_copy(src, dst, in_sem.at[n])
        for n, (src, dst) in enumerate(((c_hbm, c_ref), (p_hbm, p_ref), (w_hbm, w_ref)))
    ]
    for copy in fetch:
        copy.start()

    barrier = pltpu.get_barrier_semaphore()
    for k in range(1, 16):
        pl.semaphore_signal(barrier, inc=1, device_id=group(k), device_id_type=MESH)
    for peer in (partner, x_cross):
        pl.semaphore_signal(barrier, inc=1, device_id=peer, device_id_type=MESH)
    for k in range(1, 8):
        pl.semaphore_signal(barrier, inc=1, device_id=at(dp_peer(k), c), device_id_type=MESH)

    def prep_own(t, _):
        cols = pl.ds(pl.multiple_of(t * TILE, TILE), TILE)
        fill(bown, c_ref[:, cols], scale, True, cols)
        arow[cols, :] = bown[:, cols].T
        return 0

    def prep_pts(t, _):
        cols = pl.ds(pl.multiple_of(t * 512, 512), 512)
        for e in range(2):
            fill(bpts.at[e], p_ref[:, pl.ds(pl.multiple_of(e * (n_pts // 2) + t * 512, 512), 512)], scale, False, cols)
        return 0

    with jax.named_scope("prep"):
        fetch[0].wait()
        lax.fori_loop(0, n_cen // TILE, prep_own, 0)
        fetch[1].wait()
        lax.fori_loop(0, n_pts // 1024, prep_pts, 0)

    part = n_cen // 8
    own_part = pl.ds(pl.multiple_of(d * part, part), part)

    def place(slab, pos):
        if slab in (0, 7):
            body, at_pos = slab, pos
        else:
            first = (slab + 1) // 2 * 2 - 1
            body, at_pos = first + pos // 2, 2 * (slab - first) + pos % 2
        return zbuf.at[body, :, at_pos * part : (at_pos + 1) * part]

    def a_z(slab):
        dest = at(d, ((z + (1 if slab % 2 else 7)) % 8) * 4 + x_lo * 2 + core)
        return remote(place(max(slab - 2, 0), 0), place(slab, 0), z_send.at[slab], z_recv.at[slab], dest)

    def a_x(slab):
        return remote(place(slab, 0), place(slab, 2), x_send.at[slab], x_recv.at[slab], x_next)

    def a_core(slab):
        return remote(place(slab, 0), place(slab, 1), c1_send.at[slab], c1_recv.at[slab], partner)

    def a_cross(slab):
        if slab == 7:
            return remote(place(7, 0), place(7, 3), c3_send.at[7], c3_recv.at[7], x_cross)
        return remote(place(slab, 2), place(slab, 3), c3_send.at[slab], c3_recv.at[slab], partner)

    def z_came(slab):
        a_z(slab).wait_recv()
        if slab + 2 <= 7:
            a_z(slab + 2).start()
        a_core(slab).start()
        a_x(slab).start()
        if slab == 7:
            a_cross(slab).start()

    def x_came(slab):
        a_x(slab).wait_recv()
        a_cross(slab).start()

    def arrived(body, h):
        if body in (0, 7):
            if body == 7 and h == 1:
                a_x(7).wait_recv()
            (a_cross if h else a_core)(body).wait_recv()
        else:
            slab = (body - 1) // 2 * 2 + 1 + h
            (a_core if body % 2 else a_cross)(slab).wait_recv()

    a_own = [
        pltpu.make_async_copy(src.at[:, own_part], zbuf.at[0, lo : lo + src.shape[0], 0:part], own_sem.at[n])
        for n, (src, lo) in enumerate(((c_hbm, 0), (w_hbm, feats)))
    ]
    for copy in a_own:
        copy.start()

    def nm_cols(t):
        return pl.ds(pl.multiple_of(t * WIDE, WIDE), WIDE)

    def nm_sum(t, ref):
        fpart[ref, :, nm_cols(t)] = dot(w_ref[...], kts[ref][:, nm_cols(t)])

    def nm_sum_b(t):
        nm_sum(t, 1)

    def nm_step(t, first):
        for ref in range(2):
            right = bpts[ref, :, nm_cols(t)]
            acc = None
            for b in range(n_cen // TILE):
                rows = pl.ds(b * TILE, TILE)
                if ref or not first:
                    one = dot(w_ref[:, rows], kts[1 - ref][rows, nm_cols(t + ref - 1)])
                    acc = one if acc is None else acc + one
                kts[ref][rows, nm_cols(t)] = jnp.exp2(dot(arow[rows, :], right)).astype(BF16)
            if ref or not first:
                fpart[1 - ref, :, nm_cols(t + ref - 1)] = acc

    piece = cpts // 2

    def d1(q):
        return remote(sbuf.at[q], dbuf.at[q], d1_send.at[q], d1_recv.at[q], partner)

    def d1_go(q):
        for e in range(2):
            sbuf[q, :, e * piece : (e + 1) * piece] = fpart[e, pl.ds(r_other, half), q * piece : (q + 1) * piece].astype(BF16)
        d1(q).start()

    def rs(q, k):
        lanes = pl.ds(pl.multiple_of(chip_peer(k) * share, share), share)
        return remote(rsend.at[q, :, lanes], rrecv.at[q, k], rs_send.at[q, k], rs_recv.at[q, k], group(k))

    own_rows = pl.ds(r_own, half)

    def rs_go(q):
        d1(q).wait_recv()
        for e in range(2):
            lanes = slice(e * piece, (e + 1) * piece)
            mine = fpart[e, own_rows, q * piece : (q + 1) * piece]
            rsend[q, :, lanes] = (mine + dbuf[q, :, lanes].astype(F32)).astype(BF16)
        for k in range(1, 16):
            rs(q, k).start()

    def own_share(q):
        return (chip // 8, own_rows, pl.ds(pl.multiple_of(q * piece + (chip % 8) * share, share), share))

    def ag(q, k):
        where = fwd.at[own_share(q)]
        return remote(where, where, ag_send.at[q, k], ag_recv.at[q, k], group(k))

    def ag_go(q):
        total = rsend[q, :, pl.ds(pl.multiple_of(chip * share, share), share)].astype(F32)
        for k in range(1, 16):
            rs(q, k).wait_recv()
            total = total + rrecv[q, k].astype(F32)
        fwd[own_share(q)] = total.astype(BF16)
        for k in range(1, 16):
            ag(q, k).start()

    def d2(q):
        where = fwd.at[:, own_rows, q * piece : (q + 1) * piece]
        return remote(where, where, d2_send.at[q], d2_recv.at[q], partner)

    def d2_go(q):
        for k in range(1, 16):
            ag(q, k).wait_recv()
        d2(q).start()

    hcen = n_cen // 2
    groups = n_cen // WIDE

    def mm_sum(body, g, b, acc):
        rows = pl.ds(b * TILE, TILE)
        one = dot(zbuf[body, feats : feats + outs, rows], tiles[g % 2][rows, :])
        return one if acc is None else acc + one

    def mm_add(g, acc, first):
        cols = slice(g * WIDE, (g + 1) * WIDE)
        mmacc[:, cols] = acc if first else mmacc[:, cols] + acc

    def mm(body, first):
        for h in range(2):
            cols = slice(h * WIDE, (h + 1) * WIDE)
            fill(zaug, zbuf[body, 0:feats, cols], scale, False, cols)
            zrow[cols, :] = zaug[:, cols].T
        for g in range(groups):
            acc = None
            last = (g - 1) % groups
            for b in range(hcen // TILE):
                rows = pl.ds(b * TILE, TILE)
                if g or not first:
                    acc = mm_sum(body if g else body - 1, last, b, acc)
                tiles[g % 2][rows, :] = jnp.exp2(dot(zrow[rows, :], bown[:, g * WIDE : (g + 1) * WIDE])).astype(BF16)
            if g or not first:
                mm_add(last, acc, first)

    def actions(n, table):
        for step, todo in table.items():

            @pl.when(n == step)
            def _():
                for f, q in todo:
                    f(q)

    steps = n_pts // WIDE // 2
    fetch[2].wait()
    with jax.named_scope("nm_a"):
        nm_step(0, True)
    with jax.named_scope("barrier"):
        pl.semaphore_wait(barrier, 24)
    for copy in a_own:
        copy.wait()
    a_z(1).start()
    a_z(2).start()
    a_x(0).start()
    a_core(0).start()

    def nm_body(n, _):
        with jax.named_scope("nm_body"):
            nm_step(n, False)
        with jax.named_scope("nm_act"):
            actions(n, {1: [(nm_sum_b, 1), (d1_go, 0)], 2: [(z_came, 1), (z_came, 2), (x_came, 0), (rs_go, 0)]})
        return 0

    lax.fori_loop(1, steps, nm_body, 0)
    with jax.named_scope("nm_end"):
        nm_sum(steps - 1, 1)
    with jax.named_scope("nm_end_act"):
        d1_go(1)
        arrived(0, 0)
        arrived(0, 1)

    mmacc[:, (groups - 1) * WIDE :] = jnp.zeros((outs, WIDE), F32)
    with jax.named_scope("mm_0"):
        mm(0, True)
    with jax.named_scope("mm_0_act"):
        z_came(3)
        z_came(4)
        rs_go(1)
        x_came(1)
        x_came(2)
        arrived(1, 0)
        arrived(1, 1)

    table = {
        1: [(ag_go, 0)],
        2: [(z_came, 5), (z_came, 6), (x_came, 3), (x_came, 4)],
        3: [(ag_go, 1)],
        4: [(z_came, 7), (x_came, 5), (x_came, 6)],
        5: [(d2_go, 0)],
        6: [(d2_go, 1)],
    }

    def mm_body(n, _):
        with jax.named_scope("mm_body"):
            mm(n, False)
        with jax.named_scope("mm_act"):
            for step, todo in table.items():

                @pl.when(n == step)
                def _():
                    for f, q in todo:
                        with jax.named_scope(f"{f.__name__}_{q}"):
                            f(q)
                    with jax.named_scope(f"arrived_{step + 1}"):
                        arrived(step + 1, 0)
                        arrived(step + 1, 1)

        return 0

    lax.fori_loop(1, 8, mm_body, 0)
    with jax.named_scope("mm_end"):
        acc = None
        for b in range(hcen // TILE):
            acc = mm_sum(7, groups - 1, b, acc)
        mm_add(groups - 1, acc, False)
    with jax.named_scope("d2_wait"):
        d2(0).wait_recv()
        d2(1).wait_recv()

    hshare = dshare // 2

    def slice_of(peer, h):
        return pl.ds(pl.multiple_of(peer * dshare + h * hshare, hshare), hshare)

    def back(k, h):
        rows = slice_of(dp_peer(k), h)
        total = dot_nt(fwd[0], kta[rows, :]) + dot_nt(fwd[1], ktb[rows, :])
        return total * norm + mmacc[:, rows]

    def ds_copy(k, h):
        return remote(dsend.at[k, h], drecv.at[k, h], ds_send.at[k, h], ds_recv.at[k, h], at(dp_peer(k), c))

    def dg(k, h):
        where = outt.at[:, slice_of(d, h)]
        return remote(where, where, dg_send.at[k, h], dg_recv.at[k, h], at(dp_peer(k), c))

    def back_half(h):
        def step(t, _):
            for k in (2 * t + 1, 2 * t + 2):
                dsend[k % 8, h] = back(k, h)
            ds_copy(2 * t + 1, h).start()

            @pl.when(t < 3)
            def _():
                ds_copy(2 * t + 2, h).start()

            return 0

        lax.fori_loop(0, 4, step, 0)

    def share_out(h):
        total = dsend[0, h]
        for k in range(1, 8):
            ds_copy(k, h).wait_recv()
            total = total + drecv[k, h]
        outt[:, slice_of(d, h)] = total
        for k in range(1, 8):
            dg(k, h).start()

    for h in range(2):
        with jax.named_scope(f"back_{h}"):
            back_half(h)
    for h in range(2):
        with jax.named_scope(f"share_{h}"):
            share_out(h)

    for slab in range(8):
        if slab:
            a_z(slab).wait_send()
        a_x(slab).wait_send()
        a_core(slab).wait_send()
        a_cross(slab).wait_send()
    for q in range(CHUNKS):
        d1(q).wait_send()
        d2(q).wait_send()
        for k in range(1, 16):
            rs(q, k).wait_send()
            ag(q, k).wait_send()
    for h in range(2):
        for k in range(1, 8):
            ds_copy(k, h).wait_send()
            with jax.named_scope(f"dg_{h}_{k}"):
                dg(k, h).wait_recv()
    with jax.named_scope("out"):
        out_ref[...] = outt[...]
    for h in range(2):
        for k in range(1, 8):
            dg(k, h).wait_send()


def solution(mesh):
    def on_device(points, centers, coef):
        n_pts, feats = points.shape
        n_cen, outs = coef.shape
        cpts = n_pts // CHUNKS
        dma = pltpu.SemaphoreType.DMA

        def body(*refs):
            kernel(feats, outs, n_pts, n_cen, n_pts * 8, *refs)

        return pl.pallas_call(
            body,
            out_shape=jax.ShapeDtypeStruct((outs, n_cen), F32),
            in_specs=[pl.BlockSpec(memory_space=pltpu.HBM)] * 3,
            out_specs=pl.BlockSpec(memory_space=pltpu.VMEM),
            scratch_shapes=[
                pltpu.VMEM((feats, n_pts), BF16),
                pltpu.VMEM((feats, n_cen), BF16),
                pltpu.VMEM((outs, n_cen), BF16),
                pltpu.VMEM((2, ROWS, n_pts // 2), BF16),
                pltpu.VMEM((ROWS, n_cen), BF16),
                pltpu.VMEM((n_cen, ROWS), BF16),
                pltpu.VMEM((n_cen, n_pts // 2), BF16),
                pltpu.VMEM((n_cen, n_pts // 2), BF16),
                pltpu.VMEM((n_cen // 2, WIDE), BF16),
                pltpu.VMEM((n_cen // 2, WIDE), BF16),
                pltpu.VMEM((2, outs, n_pts // 2), F32),
                pltpu.VMEM((8, feats + outs, n_cen // 2), BF16),
                pltpu.VMEM((ROWS, n_cen // 2), BF16),
                pltpu.VMEM((n_cen // 2, ROWS), BF16),
                pltpu.VMEM((outs, n_cen), F32),
                pltpu.VMEM((2, outs, n_pts // 2), BF16),
                pltpu.VMEM((CHUNKS, outs // 2, cpts), BF16),
                pltpu.VMEM((CHUNKS, outs // 2, cpts), BF16),
                pltpu.VMEM((CHUNKS, outs // 2, cpts), BF16),
                pltpu.VMEM((CHUNKS, 16, outs // 2, cpts // 16), BF16),
                pltpu.VMEM((8, 2, outs, n_cen // 16), F32),
                pltpu.VMEM((8, 2, outs, n_cen // 16), F32),
                pltpu.VMEM((outs, n_cen), F32),
                *[dma((8,))] * 8, dma((2,)), dma((3,)),
                dma((CHUNKS,)), dma((CHUNKS,)),
                dma((CHUNKS, 16)), dma((CHUNKS, 16)),
                dma((CHUNKS, 16)), dma((CHUNKS, 16)),
                dma((CHUNKS,)), dma((CHUNKS,)),
                dma((8, 2)), dma((8, 2)),
                dma((8, 2)), dma((8, 2)),
            ],
            compiler_params=pltpu.CompilerParams(
                collective_id=0, has_side_effects=True, vmem_limit_bytes=40 * 1024 * 1024
            ),
        )(*(pltpu.with_memory_space_constraint(a.T, pltpu.HBM) for a in (points, centers, coef))).T

    in_specs = (P("dp", None), P("centers", None), P("centers", None))
    return jax.shard_map(
        on_device, mesh=mesh, in_specs=in_specs, out_specs=P("centers", None), check_vma=False
    )
```

```python
import math

import jax
import jax.numpy as jnp
import numpy as np
from jax import lax
from jax.experimental import pallas as pl
from jax.experimental.pallas import tpu as pltpu
from jax.sharding import PartitionSpec as P

F32, BF16 = jnp.float32, jnp.bfloat16
MESH = pl.DeviceIdType.MESH
ROWS = 128
TILE = 256
WIDE = 512
CHUNKS = 2
FAR_CHIPS = (8, 7, 9, 6, 10, 5, 11, 4, 12, 3, 13, 2, 14, 1, 15)
FAR_PLANES = (3, 5, 1, 7, 4, 2, 6)


def split3(x):
    a = x.astype(BF16)
    r = x - a.astype(F32)
    b = r.astype(BF16)
    return a, b, (r - b.astype(F32)).astype(BF16)


def tail_rows(pieces, first, ones):
    n = pieces[0].shape[1]
    row = lax.broadcasted_iota(jnp.int32, (32, n), 0)
    out = jnp.where((row >= ones) & (row < ones + 3), 1.0, 0.0)
    for k, piece in enumerate(pieces):
        out = jnp.where(row == first + k, piece.astype(F32), out)
    return out.astype(BF16)


def fill(dst, feats, scale, scaled, cols):
    wide = feats.astype(F32)
    squares = split3(-scale * jnp.sum(wide * wide, axis=0, keepdims=True))
    parts = split3((2.0 * scale) * wide) if scaled else (feats,) * 3
    for k in range(3):
        dst[32 * k : 32 * (k + 1), cols] = parts[k]
    dst[96:128, cols] = tail_rows(squares, 3 if scaled else 0, 0 if scaled else 3)


def dot(a, b):
    return jnp.dot(a, b, preferred_element_type=F32)


def dot_nt(a, b):
    return lax.dot_general(a, b, (((1,), (1,)), ((), ())), preferred_element_type=F32)


def kernel(
    feats, outs, n_pts, n_cen, total_pts,
    p_hbm, c_hbm, w_hbm, out_ref,
    p_ref, c_ref, w_ref,
    bpts, bown, arow, kta, ktb, tilea, tileb, fpart, zbuf, zaug, zrow, mmacc, fwd,
    sbuf, dbuf, rsend, rrecv, dsend, drecv, outt,
    z_send, z_recv, x_send, x_recv, c1_send, c1_recv, c3_send, c3_recv, own_sem, in_sem,
    d1_send, d1_recv, rs_send, rs_recv, ag_send, ag_recv,
    d2_send, d2_recv, ds_send, ds_recv, dg_send, dg_recv,
):
    scale = math.log2(math.e) * 2.0 / feats
    norm = float(np.float32(1.0) / np.sqrt(np.float32(total_pts)))
    d, c = lax.axis_index("dp"), lax.axis_index("centers")
    core, x_lo, z = c % 2, (c // 2) % 2, c // 4
    chip = c // 2
    y, x_hi = d // 2, d % 2
    kts, tiles = (kta, ktb), (tilea, tileb)
    half = outs // 2
    r_own = pl.multiple_of(half * core, half)
    r_other = pl.multiple_of(half * (1 - core), half)
    cpts = n_pts // CHUNKS
    share = cpts // 16
    dshare = n_cen // 8

    def at(dp, cen):
        return {"dp": dp, "centers": cen}

    partner = at(d, chip * 2 + 1 - core)
    x_next = at(d, z * 4 + (1 - x_lo) * 2 + core)
    x_cross = at(d, z * 4 + (1 - x_lo) * 2 + 1 - core)

    def chip_peer(k):
        return (chip + k) % 16

    def group(k):
        return at(d, chip_peer(k) * 2 + core)

    def dp_peer(k):
        return (d + k) % 8

    def remote(src, dst, send, recv, dev):
        return pltpu.make_async_remote_copy(
            src_ref=src, dst_ref=dst, send_sem=send, recv_sem=recv, device_id=dev, device_id_type=MESH
        )

    fetch = [
        pltpu.make_async_copy(src, dst, in_sem.at[n])
        for n, (src, dst) in enumerate(((c_hbm, c_ref), (p_hbm, p_ref), (w_hbm, w_ref)))
    ]
    for copy in fetch:
        copy.start()

    barrier = pltpu.get_barrier_semaphore()
    for k in range(1, 16):
        pl.semaphore_signal(barrier, inc=1, device_id=group(k), device_id_type=MESH)
    for peer in (partner, x_cross):
        pl.semaphore_signal(barrier, inc=1, device_id=peer, device_id_type=MESH)
    for k in range(1, 8):
        pl.semaphore_signal(barrier, inc=1, device_id=at(dp_peer(k), c), device_id_type=MESH)

    def prep_own(t, _):
        cols = pl.ds(pl.multiple_of(t * TILE, TILE), TILE)
        fill(bown, c_ref[:, cols], scale, True, cols)
        arow[cols, :] = bown[:, cols].T
        return 0

    def prep_pts(t, _):
        cols = pl.ds(pl.multiple_of(t * 512, 512), 512)
        for e in range(2):
            fill(bpts.at[e], p_ref[:, pl.ds(pl.multiple_of(e * (n_pts // 2) + t * 512, 512), 512)], scale, False, cols)
        return 0

    with jax.named_scope("prep"):
        fetch[0].wait()
        lax.fori_loop(0, n_cen // TILE, prep_own, 0)
        fetch[1].wait()
        lax.fori_loop(0, n_pts // 1024, prep_pts, 0)

    part = n_cen // 8
    own_part = pl.ds(pl.multiple_of(d * part, part), part)

    def place(slab, pos):
        if slab in (0, 7):
            body, at_pos = slab, pos
        else:
            first = (slab + 1) // 2 * 2 - 1
            body, at_pos = first + pos // 2, 2 * (slab - first) + pos % 2
        return zbuf.at[body, :, at_pos * part : (at_pos + 1) * part]

    def a_z(slab):
        dest = at(d, ((z + (1 if slab % 2 else 7)) % 8) * 4 + x_lo * 2 + core)
        return remote(place(max(slab - 2, 0), 0), place(slab, 0), z_send.at[slab], z_recv.at[slab], dest)

    def a_x(slab):
        return remote(place(slab, 0), place(slab, 2), x_send.at[slab], x_recv.at[slab], x_next)

    def a_core(slab):
        return remote(place(slab, 0), place(slab, 1), c1_send.at[slab], c1_recv.at[slab], partner)

    def a_cross(slab):
        if slab == 7:
            return remote(place(7, 0), place(7, 3), c3_send.at[7], c3_recv.at[7], x_cross)
        return remote(place(slab, 2), place(slab, 3), c3_send.at[slab], c3_recv.at[slab], partner)

    def z_came(slab):
        a_z(slab).wait_recv()
        if slab + 2 <= 7:
            a_z(slab + 2).start()
        a_core(slab).start()
        a_x(slab).start()
        if slab == 7:
            a_cross(slab).start()

    def x_came(slab):
        a_x(slab).wait_recv()
        a_cross(slab).start()

    def arrived(body, h):
        if body in (0, 7):
            if body == 7 and h == 1:
                a_x(7).wait_recv()
            (a_cross if h else a_core)(body).wait_recv()
        else:
            slab = (body - 1) // 2 * 2 + 1 + h
            (a_core if body % 2 else a_cross)(slab).wait_recv()

    a_own = [
        pltpu.make_async_copy(src.at[:, own_part], zbuf.at[0, lo : lo + src.shape[0], 0:part], own_sem.at[n])
        for n, (src, lo) in enumerate(((c_hbm, 0), (w_hbm, feats)))
    ]
    for copy in a_own:
        copy.start()

    def nm_cols(t):
        return pl.ds(pl.multiple_of(t * WIDE, WIDE), WIDE)

    def nm_sum(t, ref):
        fpart[ref, :, nm_cols(t)] = dot(w_ref[...], kts[ref][:, nm_cols(t)])

    def nm_sum_b(t):
        nm_sum(t, 1)

    def nm_step(t, first):
        for ref in range(2):
            right = bpts[ref, :, nm_cols(t)]
            acc = None
            for b in range(n_cen // TILE):
                rows = pl.ds(b * TILE, TILE)
                if ref or not first:
                    one = dot(w_ref[:, rows], kts[1 - ref][rows, nm_cols(t + ref - 1)])
                    acc = one if acc is None else acc + one
                kts[ref][rows, nm_cols(t)] = jnp.exp2(dot(arow[rows, :], right)).astype(BF16)
            if ref or not first:
                fpart[1 - ref, :, nm_cols(t + ref - 1)] = acc

    piece = cpts // 2

    def d1(q):
        return remote(sbuf.at[q], dbuf.at[q], d1_send.at[q], d1_recv.at[q], partner)

    def d1_go(q):
        for e in range(2):
            sbuf[q, :, e * piece : (e + 1) * piece] = fpart[e, pl.ds(r_other, half), q * piece : (q + 1) * piece].astype(BF16)
        d1(q).start()

    def rs(q, k):
        lanes = pl.ds(pl.multiple_of(chip_peer(k) * share, share), share)
        return remote(rsend.at[q, :, lanes], rrecv.at[q, k], rs_send.at[q, k], rs_recv.at[q, k], group(k))

    own_rows = pl.ds(r_own, half)

    def rs_go(q):
        d1(q).wait_recv()
        for e in range(2):
            lanes = slice(e * piece, (e + 1) * piece)
            mine = fpart[e, own_rows, q * piece : (q + 1) * piece]
            rsend[q, :, lanes] = (mine + dbuf[q, :, lanes].astype(F32)).astype(BF16)
        for k in FAR_CHIPS:
            rs(q, k).start()

    def own_share(q):
        return (chip // 8, own_rows, pl.ds(pl.multiple_of(q * piece + (chip % 8) * share, share), share))

    def ag(q, k):
        where = fwd.at[own_share(q)]
        return remote(where, where, ag_send.at[q, k], ag_recv.at[q, k], group(k))

    def ag_go(q):
        total = rsend[q, :, pl.ds(pl.multiple_of(chip * share, share), share)].astype(F32)
        for k in range(1, 16):
            rs(q, k).wait_recv()
            total = total + rrecv[q, k].astype(F32)
        fwd[own_share(q)] = total.astype(BF16)
        for k in FAR_CHIPS:
            ag(q, k).start()

    def d2(q):
        where = fwd.at[:, own_rows, q * piece : (q + 1) * piece]
        return remote(where, where, d2_send.at[q], d2_recv.at[q], partner)

    def d2_go(q):
        for k in range(1, 16):
            ag(q, k).wait_recv()
        d2(q).start()

    hcen = n_cen // 2
    groups = n_cen // WIDE

    def mm_sum(body, g, b, acc):
        rows = pl.ds(b * TILE, TILE)
        one = dot(zbuf[body, feats : feats + outs, rows], tiles[g % 2][rows, :])
        return one if acc is None else acc + one

    def mm_add(g, acc, first):
        cols = slice(g * WIDE, (g + 1) * WIDE)
        mmacc[:, cols] = acc if first else mmacc[:, cols] + acc

    def mm(body, first):
        for h in range(2):
            cols = slice(h * WIDE, (h + 1) * WIDE)
            fill(zaug, zbuf[body, 0:feats, cols], scale, False, cols)
            zrow[cols, :] = zaug[:, cols].T
        for g in range(groups):
            acc = None
            last = (g - 1) % groups
            for b in range(hcen // TILE):
                rows = pl.ds(b * TILE, TILE)
                if g or not first:
                    acc = mm_sum(body if g else body - 1, last, b, acc)
                tiles[g % 2][rows, :] = jnp.exp2(dot(zrow[rows, :], bown[:, g * WIDE : (g + 1) * WIDE])).astype(BF16)
            if g or not first:
                mm_add(last, acc, first)

    def actions(n, table):
        for step, todo in table.items():

            @pl.when(n == step)
            def _():
                for f, q in todo:
                    f(q)

    steps = n_pts // WIDE // 2
    fetch[2].wait()
    with jax.named_scope("nm_a"):
        nm_step(0, True)
    with jax.named_scope("barrier"):
        pl.semaphore_wait(barrier, 24)
    for copy in a_own:
        copy.wait()
    a_z(1).start()
    a_z(2).start()
    a_x(0).start()
    a_core(0).start()

    def nm_body(n, _):
        with jax.named_scope("nm_body"):
            nm_step(n, False)
        with jax.named_scope("nm_act"):
            actions(n, {1: [(nm_sum_b, 1), (d1_go, 0)], 2: [(z_came, 1), (z_came, 2), (x_came, 0), (rs_go, 0)]})
        return 0

    lax.fori_loop(1, steps, nm_body, 0)
    with jax.named_scope("nm_end"):
        nm_sum(steps - 1, 1)
    with jax.named_scope("nm_end_act"):
        d1_go(1)
        arrived(0, 0)
        arrived(0, 1)

    mmacc[:, (groups - 1) * WIDE :] = jnp.zeros((outs, WIDE), F32)
    with jax.named_scope("mm_0"):
        mm(0, True)
    with jax.named_scope("mm_0_act"):
        z_came(3)
        z_came(4)
        rs_go(1)
        x_came(1)
        x_came(2)
        arrived(1, 0)
        arrived(1, 1)

    table = {
        1: [(ag_go, 0)],
        2: [(z_came, 5), (z_came, 6), (x_came, 3), (x_came, 4)],
        3: [(ag_go, 1)],
        4: [(z_came, 7), (x_came, 5), (x_came, 6)],
        5: [(d2_go, 0)],
        6: [(d2_go, 1)],
    }

    def mm_body(n, _):
        with jax.named_scope("mm_body"):
            mm(n, False)
        with jax.named_scope("mm_act"):
            for step, todo in table.items():

                @pl.when(n == step)
                def _():
                    for f, q in todo:
                        with jax.named_scope(f"{f.__name__}_{q}"):
                            f(q)
                    with jax.named_scope(f"arrived_{step + 1}"):
                        arrived(step + 1, 0)
                        arrived(step + 1, 1)

        return 0

    lax.fori_loop(1, 8, mm_body, 0)
    with jax.named_scope("mm_end"):
        acc = None
        for b in range(hcen // TILE):
            acc = mm_sum(7, groups - 1, b, acc)
        mm_add(groups - 1, acc, False)
    with jax.named_scope("d2_wait"):
        d2(0).wait_recv()
        d2(1).wait_recv()

    hshare = dshare // 2

    def slice_of(peer, h):
        return pl.ds(pl.multiple_of(peer * dshare + h * hshare, hshare), hshare)

    def back(k, h):
        rows = slice_of(dp_peer(k), h)
        total = dot_nt(fwd[0], kta[rows, :]) + dot_nt(fwd[1], ktb[rows, :])
        return total * norm + mmacc[:, rows]

    def ds_copy(k, h):
        return remote(dsend.at[k, h], drecv.at[k, h], ds_send.at[k, h], ds_recv.at[k, h], at(dp_peer(k), c))

    def dg(k, h):
        where = outt.at[:, slice_of(d, h)]
        return remote(where, where, dg_send.at[k, h], dg_recv.at[k, h], at(dp_peer(k), c))

    def back_half(h):
        def step(t, _):
            for k in (2 * t + 1, 2 * t + 2):
                dsend[k % 8, h] = back(k, h)
            ds_copy(2 * t + 1, h).start()

            @pl.when(t < 3)
            def _():
                ds_copy(2 * t + 2, h).start()

            return 0

        lax.fori_loop(0, 4, step, 0)

    def share_out(h):
        total = dsend[0, h]
        for k in range(1, 8):
            ds_copy(k, h).wait_recv()
            total = total + drecv[k, h]
        outt[:, slice_of(d, h)] = total
        for k in FAR_PLANES:
            dg(k, h).start()

    for h in range(2):
        with jax.named_scope(f"back_{h}"):
            back_half(h)
    for h in range(2):
        with jax.named_scope(f"share_{h}"):
            share_out(h)

    for slab in range(8):
        if slab:
            a_z(slab).wait_send()
        a_x(slab).wait_send()
        a_core(slab).wait_send()
        a_cross(slab).wait_send()
    for q in range(CHUNKS):
        d1(q).wait_send()
        d2(q).wait_send()
        for k in range(1, 16):
            rs(q, k).wait_send()
            ag(q, k).wait_send()
    for h in range(2):
        for k in range(1, 8):
            ds_copy(k, h).wait_send()
            with jax.named_scope(f"dg_{h}_{k}"):
                dg(k, h).wait_recv()
    with jax.named_scope("out"):
        out_ref[...] = outt[...]
    for h in range(2):
        for k in range(1, 8):
            dg(k, h).wait_send()


def solution(mesh):
    def on_device(points, centers, coef):
        n_pts, feats = points.shape
        n_cen, outs = coef.shape
        cpts = n_pts // CHUNKS
        dma = pltpu.SemaphoreType.DMA

        def body(*refs):
            kernel(feats, outs, n_pts, n_cen, n_pts * 8, *refs)

        return pl.pallas_call(
            body,
            out_shape=jax.ShapeDtypeStruct((outs, n_cen), F32),
            in_specs=[pl.BlockSpec(memory_space=pltpu.HBM)] * 3,
            out_specs=pl.BlockSpec(memory_space=pltpu.VMEM),
            scratch_shapes=[
                pltpu.VMEM((feats, n_pts), BF16),
                pltpu.VMEM((feats, n_cen), BF16),
                pltpu.VMEM((outs, n_cen), BF16),
                pltpu.VMEM((2, ROWS, n_pts // 2), BF16),
                pltpu.VMEM((ROWS, n_cen), BF16),
                pltpu.VMEM((n_cen, ROWS), BF16),
                pltpu.VMEM((n_cen, n_pts // 2), BF16),
                pltpu.VMEM((n_cen, n_pts // 2), BF16),
                pltpu.VMEM((n_cen // 2, WIDE), BF16),
                pltpu.VMEM((n_cen // 2, WIDE), BF16),
                pltpu.VMEM((2, outs, n_pts // 2), F32),
                pltpu.VMEM((8, feats + outs, n_cen // 2), BF16),
                pltpu.VMEM((ROWS, n_cen // 2), BF16),
                pltpu.VMEM((n_cen // 2, ROWS), BF16),
                pltpu.VMEM((outs, n_cen), F32),
                pltpu.VMEM((2, outs, n_pts // 2), BF16),
                pltpu.VMEM((CHUNKS, outs // 2, cpts), BF16),
                pltpu.VMEM((CHUNKS, outs // 2, cpts), BF16),
                pltpu.VMEM((CHUNKS, outs // 2, cpts), BF16),
                pltpu.VMEM((CHUNKS, 16, outs // 2, cpts // 16), BF16),
                pltpu.VMEM((8, 2, outs, n_cen // 16), F32),
                pltpu.VMEM((8, 2, outs, n_cen // 16), F32),
                pltpu.VMEM((outs, n_cen), F32),
                *[dma((8,))] * 8, dma((2,)), dma((3,)),
                dma((CHUNKS,)), dma((CHUNKS,)),
                dma((CHUNKS, 16)), dma((CHUNKS, 16)),
                dma((CHUNKS, 16)), dma((CHUNKS, 16)),
                dma((CHUNKS,)), dma((CHUNKS,)),
                dma((8, 2)), dma((8, 2)),
                dma((8, 2)), dma((8, 2)),
            ],
            compiler_params=pltpu.CompilerParams(
                collective_id=0, has_side_effects=True, vmem_limit_bytes=40 * 1024 * 1024
            ),
        )(*(pltpu.with_memory_space_constraint(a.T, pltpu.HBM) for a in (points, centers, coef))).T

    in_specs = (P("dp", None), P("centers", None), P("centers", None))
    return jax.shard_map(
        on_device, mesh=mesh, in_specs=in_specs, out_specs=P("centers", None), check_vma=False
    )
```
